256 devices in a mesh: seq: 16 (over x, y_hi, core), batch: 16 (over y_lo, z).
Axes of the slice: x: 4, y: 4 (y_hi: 2, y_lo: 2; y = y_hi * 2 + y_lo), z: 8, core: 2. Of those that a mesh axis runs over, the one named last changes fastest.
Arguments:
- query_rows: bfloat16 [16, 2048, 2048], P('batch', 'seq'), may hold values from -6 to 6, as said below
- key_rows: bfloat16 [16, 2048, 1024], P('batch', 'seq'), may hold values from -6 to 6, as said below
- value_rows: bfloat16 [16, 2048, 1024], P('batch', 'seq'), may hold values from -6 to 6, as said below
- attn_output: bfloat16 [16, 2048, 2048], P('batch', 'seq'), may hold values from -6 to 6, as said below
- output_grad: bfloat16 [16, 2048, 2048], P('batch', 'seq'), may hold values from -6 to 6
- log_norm: float32 [16, 16, 2048], P('batch', None, 'seq'), as said below
- slab_order: int32 [16, 16], P('batch', 'seq'), may hold values from 0 to 15, as said below
- normed_input: bfloat16 [16, 2048, 4608], P('batch', 'seq'), may hold values from -6 to 6
Outputs:
- grad_query: bfloat16 [16, 2048, 2048], P('batch', 'seq')
- grad_key: bfloat16 [16, 2048, 1024], P('batch', 'seq')
- grad_weight: float32 [4608, 1024], P('seq')
The draws below stay inside these ranges and needn't reach their ends.
Inputs may be any that keep to these rules, and one draw needn't show every extreme that they name: `query_rows`: queries of a causal forward pass with 16 heads. `key_rows`: keys of the same forward pass with 8 heads. `value_rows`: values of the same forward pass. `attn_output`: the forward pass's output: for each head, sum over keys at or before the query's position of exp(score - log_norm) times the value. `log_norm`: log of the sum of exp(score) over the keys at or before the query's position, so that each row's weights sum to one. `slab_order`: each row is a permutation of the slab places.
All inputs are finite; a program needn't handle non-finite values.
Results may differ from the reference program's by a relative error of at most 0.025.
Values may be sent and summed in bfloat16 or wider, within the bound.
A program may use at most 128 MiB of HBM per device.

```python
import jax
import jax.numpy as jnp
from jax import lax

D = 4608
HEADS = 16
KV_HEADS = 8
HEAD = 128
TOK_DEV = 128
LENGTH = 2048
BATCH = 16


SCALE = 144.0 ** (-0.5)


def slab_places(key):
    base = jax.random.fold_in(key, 11)
    subkeys = jax.random.split(base, BATCH)
    return jax.vmap(lambda subkey: jax.random.permutation(subkey, LENGTH // TOK_DEV))(subkeys).astype(jnp.int32)


def one_draw(subkey, width):
    values = jax.random.normal(subkey, (BATCH, LENGTH, width), jnp.float32)
    return jnp.clip(values, -6.0, 6.0).astype(jnp.bfloat16)


def projections(key):
    base = jax.random.fold_in(key, 23)
    first, second, third = jax.random.split(base, 3)
    return (one_draw(first, HEADS * HEAD), one_draw(second, KV_HEADS * HEAD), one_draw(third, KV_HEADS * HEAD))


def forward(key):
    queries, keys, values = projections(key)
    order = slab_places(key)
    group = HEADS // KV_HEADS

    def sequence(inputs):
        query_seq, key_seq, value_seq, order_row = inputs
        positions = (order_row[:, None] * TOK_DEV + jnp.arange(TOK_DEV, dtype=jnp.int32)[None, :]).reshape(LENGTH)
        query_f = query_seq.astype(jnp.float32).reshape(LENGTH, KV_HEADS, group, HEAD)
        key_f = key_seq.astype(jnp.float32).reshape(LENGTH, KV_HEADS, HEAD)
        value_f = value_seq.astype(jnp.float32).reshape(LENGTH, KV_HEADS, HEAD)
        scores = SCALE * jnp.einsum('tgrd,kgd->grtk', query_f, key_f)
        allowed = positions[None, :] <= positions[:, None]
        scores = jnp.where(allowed, scores, -1e+30)
        top = jnp.max(scores, axis=3, keepdims=True)
        weights = jnp.where(allowed, jnp.exp(scores - top), 0.0)
        total = jnp.sum(weights, axis=3, keepdims=True)
        outputs = jnp.einsum('grtk,kgd->tgrd', weights / total, value_f)
        norms = (top + jnp.log(total))[..., 0].reshape(HEADS, LENGTH)
        return (outputs.reshape(LENGTH, HEADS * HEAD).astype(jnp.bfloat16), norms)
    return lax.map(sequence, (queries, keys, values, order))


def draw_query_rows(key, part):
    return projections(key)[0]


def draw_key_rows(key, part):
    return projections(key)[1]


def draw_value_rows(key, part):
    return projections(key)[2]


def draw_attn_output(key, part):
    return forward(key)[0]


def draw_log_norm(key, part):
    return forward(key)[1]


def draw_slab_order(key, part):
    return slab_places(key)


def level_of(own_key, shape, shards, smallest, top_value):
    level = 1.0
    for dim, blocks in shards:
        heights = jax.random.uniform(jax.random.fold_in(jax.random.fold_in(own_key, 6), dim), (blocks,), jnp.float32, smallest / len(shards), top_value / len(shards))
        level = level * jnp.repeat(jnp.exp(heights), shape[dim] // blocks).reshape((-1,) + (1,) * (len(shape) - 1 - dim))
    return level


def scatter_about(stream_key, extent, scale, limit, shards=(), kind=jnp.bfloat16):
    drawn = jax.random.normal(stream_key, extent, jnp.float32) * scale
    if len(shards) > 0:
        drawn = level_of(stream_key, extent, shards, -0.22, 0.18) * drawn
    return jnp.clip(drawn, min=-limit, max=limit).astype(kind)


def setup_inputs(seed: int = 0) -> dict:
    seeds = jax.random.split(jax.random.key(seed), 9)
    return {
        "query_rows": draw_query_rows(jax.random.fold_in(seeds[8], 71), 0),
        "key_rows": draw_key_rows(jax.random.fold_in(seeds[8], 71), 0),
        "value_rows": draw_value_rows(jax.random.fold_in(seeds[8], 71), 0),
        "attn_output": draw_attn_output(jax.random.fold_in(seeds[8], 71), 0),
        "output_grad": scatter_about(seeds[4], (BATCH, LENGTH, HEADS * HEAD), 1.0, 6.0, ((0, 16), (1, 16))),
        "log_norm": draw_log_norm(jax.random.fold_in(seeds[8], 71), 0),
        "slab_order": draw_slab_order(jax.random.fold_in(seeds[8], 71), 0),
        "normed_input": scatter_about(seeds[7], (BATCH, LENGTH, D), 1.0, 6.0, ((0, 16), (1, 16))),
    }


SCALE = 144.0 ** -0.5


def rounded(values):
    return lax.optimization_barrier(values.astype(jnp.bfloat16)).astype(jnp.float32)


def block_terms(query_rows, output_rows, grad_rows, norm_rows, query_pos, key_rows, value_rows, key_pos):
    count = query_rows.shape[0]
    keys_count = key_rows.shape[0]
    group = HEADS // KV_HEADS
    queries = query_rows.astype(jnp.float32).reshape(count, KV_HEADS, group, HEAD)
    grads = grad_rows.astype(jnp.float32).reshape(count, KV_HEADS, group, HEAD)
    outputs = output_rows.astype(jnp.float32).reshape(count, KV_HEADS, group, HEAD)
    keys = key_rows.astype(jnp.float32).reshape(keys_count, KV_HEADS, HEAD)
    values = value_rows.astype(jnp.float32).reshape(keys_count, KV_HEADS, HEAD)
    norms = norm_rows.reshape(KV_HEADS, group, count)
    delta = jnp.transpose(jnp.sum(grads * outputs, axis=3), (1, 2, 0))
    scores = SCALE * jnp.einsum('tgrd,kgd->grtk', queries, keys)
    allowed = key_pos[None, :] <= query_pos[:, None]
    probs = jnp.where(allowed, jnp.exp(scores - norms[..., None]), 0.0)
    dprob = jnp.einsum('tgrd,kgd->grtk', grads, values)
    dscore = probs * (dprob - delta[..., None])
    probs_low = rounded(probs)
    dscore_low = rounded(dscore)
    grad_q = SCALE * jnp.einsum('grtk,kgd->tgrd', dscore_low, keys)
    grad_k = SCALE * jnp.einsum('grtk,tgrd->kgd', dscore_low, queries)
    grad_v = jnp.einsum('grtk,tgrd->kgd', probs_low, grads)
    return (grad_q.reshape(count, HEADS * HEAD),
            grad_k.reshape(keys_count, KV_HEADS * HEAD),
            grad_v.reshape(keys_count, KV_HEADS * HEAD))


def reference(query_rows, key_rows, value_rows, attn_output, output_grad, log_norm, slab_order, normed_input):
    slabs = LENGTH // TOK_DEV
    kv_width = KV_HEADS * HEAD

    def sequence(weight, inputs):
        queries, keys, values, outputs, grads, norms, order, normed = inputs
        positions = (order[:, None].astype(jnp.int32) * TOK_DEV
                     + jnp.arange(TOK_DEV, dtype=jnp.int32)[None, :]).reshape(LENGTH)

        def per_slab(carry, index):
            acc_key, acc_value = carry
            start = (index * TOK_DEV).astype(jnp.int32)
            grad_q, grad_k, grad_v = block_terms(
                lax.dynamic_slice_in_dim(queries, start, TOK_DEV, 0),
                lax.dynamic_slice_in_dim(outputs, start, TOK_DEV, 0),
                lax.dynamic_slice_in_dim(grads, start, TOK_DEV, 0),
                lax.dynamic_slice_in_dim(norms, start, TOK_DEV, 1),
                lax.dynamic_slice_in_dim(positions, start, TOK_DEV, 0),
                keys, values, positions)
            return (acc_key + rounded(grad_k), acc_value + rounded(grad_v)), grad_q.astype(jnp.bfloat16)

        zeros = jnp.zeros((LENGTH, kv_width), jnp.float32)
        (acc_key, acc_value), slab_query = lax.scan(per_slab, (zeros, zeros), jnp.arange(slabs, dtype=jnp.int32))
        grad_query = slab_query.reshape(LENGTH, HEADS * HEAD)
        grad_key = acc_key.astype(jnp.bfloat16)
        grad_value = acc_value.astype(jnp.bfloat16).astype(jnp.float32)

        def per_weight(total, index):
            start = (index * TOK_DEV).astype(jnp.int32)
            rows_in = lax.dynamic_slice_in_dim(normed, start, TOK_DEV, 0).astype(jnp.float32)
            rows_grad = lax.dynamic_slice_in_dim(grad_value, start, TOK_DEV, 0)
            part = jnp.dot(rows_in.T, rows_grad, preferred_element_type=jnp.float32)
            return total + rounded(part), None

        weight, _ = lax.scan(per_weight, weight, jnp.arange(slabs, dtype=jnp.int32))
        return weight, (grad_query, grad_key)

    start_weight = jnp.zeros((D, kv_width), jnp.float32)
    weight, (grad_query, grad_key) = lax.scan(
        sequence, start_weight,
        (query_rows, key_rows, value_rows, attn_output, output_grad, log_norm, slab_order, normed_input))
    return grad_query, grad_key, weight
```

```python
import functools

import jax
import jax.numpy as jnp
from jax import lax
from jax.experimental import pallas as pl
from jax.experimental.pallas import tpu as pltpu
from jax.sharding import PartitionSpec as P

HEADS = 16
KV_HEADS = 8
HEAD = 128
TOK = 128
D = 4608
XROWS = D // 4
QROWS = D // 16
HALF = QROWS // 2

SCALE = 144.0 ** (-0.5)
LOG2E = 1.4426950408889634

MESH = pl.DeviceIdType.MESH
F32 = jnp.float32
BF16 = jnp.bfloat16

RELS = ((1, 0), (1, 1), (3, 0), (3, 1), (2, 0), (2, 1), (0, 1))
STEPS = (1, 3, 2)


def dot(a, b):
    return lax.dot_general(a, b, (((1,), (0,)), ((), ())), preferred_element_type=F32)


def dot_nt(a, b):
    return lax.dot_general(a, b, (((1,), (1,)), ((), ())), preferred_element_type=F32)


def kernel(
    q_ref, do_ref, o_ref, k_ref, v_ref, ln_ref, slab_ref, n_ref,
    gq_ref, gk_ref, w_ref,
    pos_s, pos_r, aux_s, aux_r, q_r, do_r, kv_r, nt_s, nt_r, kt, dqt, acc, dkv_s, dkv_r,
    dvg, dq_s, dk_s, wy_s, wy_r, wz_s, wz_r, wa_s, wf,
    x_ss, x_rs, x_ls, y_ss, y_rs, n_ss, n_rs, n_ls, p_ss, p_rs, dy_ss, dy_rs, dv_ss, dv_rs,
    g_ss, g_rs, g_ls, wy_ss, wy_rs, wz_ss, wz_rs, wa_ss, wa_rs,
):
    seq = lax.axis_index("seq")
    batch = lax.axis_index("batch")
    x, yh, c = seq // 4, (seq // 2) % 2, seq % 2
    yl, z = batch // 8, batch % 8
    y = 2 * yh + yl

    def device(x_, y_, c_, z_):
        return {"seq": 4 * x_ + 2 * (y_ // 2) + c_, "batch": 8 * (y_ % 2) + z_}

    def along_x(step):
        return (x + step) % 4

    def remote(src, dst, ss, rs, to):
        copy = pltpu.make_async_remote_copy(
            src_ref=src, dst_ref=dst, send_sem=ss, recv_sem=rs,
            device_id=to, device_id_type=MESH,
        )
        copy.start()
        return copy

    def keep(src, dst, sem):
        copy = pltpu.make_async_copy(src, dst, sem)
        copy.start()
        return copy

    g = 2 * x + c
    partner = device(x, (y + 2) % 4, c, z)
    peers = [device(along_x(dx), y, (c + dc) % 2, z) for dx, dc in RELS]
    slots = [2 * along_x(dx) + (c + dc) % 2 for dx, dc in RELS]
    sources = [2 * along_x(4 - dx) + (c + dc) % 2 for dx, dc in RELS]

    pos_s[...] = jnp.full((8, TOK), slab_ref[0, 0] * TOK, jnp.int32).astype(F32)

    barrier = pltpu.get_barrier_semaphore()
    for to in peers:
        pl.semaphore_signal(barrier, inc=1, device_id=to, device_id_type=MESH)
    for step in STEPS:
        to = device(x, (y + step) % 4, c, z)
        pl.semaphore_signal(barrier, inc=1, device_id=to, device_id_type=MESH)
    for dyl in range(2):
        for dc in range(2):
            for dz in range(8):
                if dyl + dc + dz > 0:
                    to = device(x, 2 * yh + (yl + dyl) % 2, (c + dc) % 2, (z + dz) % 8)
                    pl.semaphore_signal(barrier, inc=1, device_id=to, device_id_type=MESH)
    pl.semaphore_wait(barrier, 41)

    sent = []

    def columns(ref, slot, width):
        return ref.at[:, pl.ds(pl.multiple_of(slot * width, width), width)]

    first, own_first = [], [
        keep(columns(k_ref, g, HEAD), kv_r.at[0, 0, g], x_ls.at[0]),
        keep(columns(v_ref, g, HEAD), kv_r.at[0, 1, g], x_ls.at[1]),
        keep(pos_s, pos_r.at[0, g], x_ls.at[2]),
    ]
    for r, to in enumerate(peers):
        first.append([
            remote(columns(k_ref, slots[r], HEAD), kv_r.at[0, 0, g], x_ss.at[0, r], x_rs.at[0, r], to),
            remote(columns(v_ref, slots[r], HEAD), kv_r.at[0, 1, g], x_ss.at[1, r], x_rs.at[1, r], to),
            remote(pos_s, pos_r.at[0, g], x_ss.at[2, r], x_rs.at[2, r], to),
        ])

    def delta_of(h, carry):
        rows = []
        for e in range(2):
            at = pl.ds(pl.multiple_of((2 * h + e) * HEAD, HEAD), HEAD)
            both = do_ref[:, at].astype(F32) * o_ref[:, at].astype(F32)
            rows.append(jnp.sum(both.T, axis=0, keepdims=True))
        norms = ln_ref[pl.ds(2 * h, 2), :] * LOG2E
        aux_s[h] = jnp.concatenate([norms, *rows, jnp.zeros((4, TOK), F32)], axis=0)
        return carry

    lax.fori_loop(0, KV_HEADS, delta_of, 0)

    second, own_second = [], [
        keep(aux_s.at[g], aux_r.at[g], x_ls.at[3]),
        keep(columns(q_ref, g, 2 * HEAD), q_r.at[g], x_ls.at[4]),
        keep(columns(do_ref, g, 2 * HEAD), do_r.at[g], x_ls.at[5]),
    ]
    for r, to in enumerate(peers):
        second.append([
            remote(columns(q_ref, slots[r], 2 * HEAD), q_r.at[g], x_ss.at[4, r], x_rs.at[4, r], to),
            remote(columns(do_ref, slots[r], 2 * HEAD), do_r.at[g], x_ss.at[5, r], x_rs.at[5, r], to),
            remote(aux_s.at[slots[r]], aux_r.at[g], x_ss.at[3, r], x_rs.at[3, r], to),
        ])

    passed = []

    def pass_on(slot, r):
        passed.append(remote(kv_r.at[0, :, slot], kv_r.at[1, :, slot], y_ss.at[0, r], y_rs.at[0, r], partner))
        passed.append(remote(pos_r.at[0, slot], pos_r.at[1, slot], y_ss.at[1, r], y_rs.at[1, r], partner))

    for copy in own_first:
        copy.wait()
    pass_on(g, 7)

    def turn(b, carry):
        at = pl.ds(pl.multiple_of(b * 128, 128), 128)
        nt_s[at, :] = n_ref[:, at].astype(F32).T.astype(BF16)
        return carry

    lax.fori_loop(0, D // 128, turn, 0)

    for r in range(7):
        for copy in first[r]:
            copy.wait_recv()
        pass_on(sources[r], r)

    def x_rows(step):
        return nt_s.at[pl.ds(pl.multiple_of(along_x(step) * XROWS, 128), XROWS), :]

    inputs = [keep(x_rows(0), nt_r.at[g], n_ls)]
    for i, step in enumerate(STEPS):
        inputs.append(
            remote(x_rows(step), nt_r.at[g], n_ss.at[i], n_rs.at[i], device(along_x(step), y, c, z))
        )

    for copy in own_second:
        copy.wait()
    for r in range(7):
        for copy in second[r]:
            copy.wait_recv()
    for copy in passed:
        copy.wait_recv()

    lane = lax.broadcasted_iota(jnp.int32, (1, TOK), 1).astype(F32)
    key_at = lax.broadcasted_iota(jnp.int32, (TOK, TOK), 0).astype(F32)

    def block(half, b, fresh):
        for k in range(4):
            kt[:, 128 * k : 128 * k + 128] = kv_r[half, 0, 4 * b + k].astype(F32).T.astype(BF16)
        acc[half] = jnp.zeros((2, 512, HEAD), F32)

        def step(j, carry):
            queries = jnp.concatenate([q_r[j, :, :HEAD], q_r[j, :, HEAD:]], axis=0)
            grads = jnp.concatenate([do_r[j, :, :HEAD], do_r[j, :, HEAD:]], axis=0)
            aux = aux_r[j]
            norms = jnp.concatenate([aux[0:1], aux[1:2]], axis=1)
            delta = jnp.concatenate([aux[2:3], aux[3:4]], axis=1)
            query_pos = pos_r[0, j][0:1] + lane
            keys = kv_r[half, 0, 4 * b : 4 * b + 4].reshape(512, HEAD)
            values = kv_r[half, 1, 4 * b : 4 * b + 4].reshape(512, HEAD)
            scores = dot_nt(keys, queries)
            dprob = dot_nt(values, grads)
            probs, dscores = [], []
            for k in range(4):
                rows = slice(128 * k, 128 * k + 128)
                ahead = query_pos - pos_r[half, 4 * b + k][0:1]
                allowed = ahead >= key_at
                prob = jnp.exp2(scores[rows] * (SCALE * LOG2E) - norms)
                prob = jnp.concatenate(
                    [jnp.where(allowed, prob[:, :128], 0.0), jnp.where(allowed, prob[:, 128:], 0.0)], axis=1
                )
                probs.append(prob.astype(BF16))
                dscores.append((prob * (dprob[rows] - delta)).astype(BF16))
            prob = jnp.concatenate(probs, axis=0)
            dscore = jnp.concatenate(dscores, axis=0)
            acc[half, 0] += dot(dscore, queries)
            acc[half, 1] += dot(prob, grads)
            term = dot(kt[...], dscore)
            if fresh:
                dqt[j] = term
            else:
                dqt[j] += term
            return carry

        lax.fori_loop(0, 8, step, 0)

    across = []
    for b in range(2):
        block(1, b, b == 0)
        dkv_s[b] = acc[1].astype(BF16)
        across.append(remote(dkv_s.at[b], dkv_r.at[b], dy_ss.at[b], dy_rs.at[b], partner))

    values_out = []
    for b in range(2):
        block(0, b, False)
        if b == 0:
            for copy in inputs:
                if copy is inputs[0]:
                    copy.wait()
                else:
                    copy.wait_recv()
            shared = []
            other = device(x, y, (c + 1) % 2, z)
            for i in range(4):
                j = 2 * along_x(i) + c
                shared.append(remote(nt_r.at[j], nt_r.at[j], p_ss.at[i], p_rs.at[i], other))
        across[b].wait_recv()
        rows = slice(512 * b, 512 * b + 512)
        dvg[0, rows] = (acc[0, 1] + dkv_r[b, 1].astype(F32)).astype(BF16)
        for i, step in enumerate(STEPS):
            values_out.append(
                remote(
                    dvg.at[0, rows], dvg.at[i + 1, rows], dv_ss.at[b, i], dv_rs.at[b, i],
                    device(along_x(step), y, c, z),
                )
            )
        keys_done = (SCALE * (acc[0, 0] + dkv_r[b, 0].astype(F32))).astype(BF16)
        dk_s[4 * b : 4 * b + 4] = keys_done.reshape(4, 128, HEAD)

    def queries_done(j, carry):
        dq_s[j] = jnp.concatenate(
            [(SCALE * dqt[j, :, :128]).T, (SCALE * dqt[j, :, 128:]).T], axis=1
        ).astype(BF16)
        return carry

    lax.fori_loop(0, 8, queries_done, 0)

    back = [
        keep(dk_s.at[g], columns(gk_ref, g, HEAD), g_ls.at[0]),
        keep(dq_s.at[g], columns(gq_ref, g, 2 * HEAD), g_ls.at[1]),
    ]
    for r, to in enumerate(peers):
        back.append(remote(dk_s.at[slots[r]], columns(gk_ref, g, HEAD), g_ss.at[0, r], g_rs.at[0, r], to))
        back.append(remote(dq_s.at[slots[r]], columns(gq_ref, g, 2 * HEAD), g_ss.at[1, r], g_rs.at[1, r], to))

    for copy in shared:
        copy.wait_recv()

    over_y = []

    def multiply(i):
        if i > 0:
            values_out[i - 1].wait_recv()
            values_out[i + 2].wait_recv()

        def quarter(t, carry):
            at = pl.ds(pl.multiple_of(t * QROWS, 32), QROWS)
            total = None
            for j in range(4):
                left = jnp.concatenate([nt_r[2 * j, at, :], nt_r[2 * j + 1, at, :]], axis=1)
                term = dot(left, dvg[i, 256 * j : 256 * j + 256])
                total = term if total is None else total + term
            wy_s[i, t] = total.astype(BF16)
            return carry

        lax.fori_loop(0, 4, quarter, 0)
        over_y.append([
            remote(
                wy_s.at[i, (y + step) % 4], wy_r.at[i, k], wy_ss.at[i, k], wy_rs.at[i, k],
                device(x, (y + step) % 4, c, z),
            )
            for k, step in enumerate(STEPS)
        ])

    def z_copy(i, r):
        return pltpu.make_async_remote_copy(
            src_ref=wz_s.at[i, r], dst_ref=wz_r.at[z], send_sem=wz_ss.at[i, r], recv_sem=wz_rs.at[z],
            device_id=device(x, y, c, 2 * i + r), device_id_type=MESH,
        )

    def reduce_y(i):
        total = wy_s[i, y].astype(F32)
        for k in range(3):
            over_y[i][k].wait_recv()
            total = total + wy_r[i, k].astype(F32)
        wz_s[i] = total.astype(BF16).reshape(2, HALF, HEAD)
        for r in range(2):
            pl.when(z != 2 * i + r)(lambda: z_copy(i, r).start())

    def w_copy(i, t):
        dyl, dz = t // 8, t % 8
        r = z % 2
        block = 2 * along_x((0, 3, 1, 2)[i]) + c
        return pltpu.make_async_remote_copy(
            src_ref=wa_s, dst_ref=wf.at[block, r], send_sem=wa_ss.at[t], recv_sem=wa_rs.at[block, r],
            device_id=device(x, 2 * yh + (yl + dyl) % 2, yl, (z + dz) % 8), device_id_type=MESH,
        )

    def w_keep(i):
        r = z % 2
        block = 2 * along_x((0, 3, 1, 2)[i]) + c
        return pltpu.make_async_copy(wa_s, wf.at[block, r], wa_rs.at[block, r])

    def reduce_z(i):
        @pl.when(z // 2 == i)
        def _():
            total = wz_s[i, z % 2].astype(F32)
            for k in range(1, 8):
                source = (z + k) % 8
                pltpu.make_async_remote_copy(
                    src_ref=wz_s.at[i, 0], dst_ref=wz_r.at[source], send_sem=wz_ss.at[i, 0],
                    recv_sem=wz_rs.at[source], device_id=device(x, y, c, source), device_id_type=MESH,
                ).wait_recv()
                total = total + wz_r[source].astype(F32)
            wa_s[...] = total.astype(BF16)
            for t in range(1, 16):
                w_copy(i, t).start()
            pl.when(c != yl)(lambda: w_copy(i, 0).start())
            pl.when(c == yl)(lambda: w_keep(i).start())

    multiply(0)
    multiply(1)
    reduce_y(0)
    multiply(2)
    reduce_y(1)
    reduce_z(0)
    multiply(3)
    reduce_y(2)
    reduce_z(1)
    reduce_y(3)
    reduce_z(2)
    reduce_z(3)

    for copy in back:
        if copy is back[0] or copy is back[1]:
            copy.wait()
        else:
            copy.wait_recv()

    for block in range(KV_HEADS):
        for r in range(2):
            pltpu.make_async_copy(wa_s, wf.at[block, r], wa_rs.at[block, r]).wait()
            w_ref[HALF * r : HALF * r + HALF, 128 * block : 128 * block + 128] = wf[block, r].astype(F32)

    for group in first + second + over_y:
        for copy in group:
            copy.wait_send()
    for copy in passed + inputs[1:] + shared + across + values_out + back[2:]:
        copy.wait_send()
    for i in range(4):
        for r in range(2):
            pl.when(z != 2 * i + r)(lambda: z_copy(i, r).wait_send())

        @pl.when(z // 2 == i)
        def _():
            for t in range(1, 16):
                w_copy(i, t).wait_send()
            pl.when(c != yl)(lambda: w_copy(i, 0).wait_send())


def local(
    query_rows, key_rows, value_rows, attn_output, output_grad, log_norm, slab_order, normed_input
):
    vmem = pl.BlockSpec(memory_space=pltpu.VMEM)
    smem = pl.BlockSpec(memory_space=pltpu.SMEM)
    dma = pltpu.SemaphoreType.DMA
    grad_query, grad_key, weight = pl.pallas_call(
        kernel,
        name="step",
        out_shape=(
            jax.ShapeDtypeStruct((TOK, HEADS * HEAD), BF16),
            jax.ShapeDtypeStruct((TOK, KV_HEADS * HEAD), BF16),
            jax.ShapeDtypeStruct((QROWS, KV_HEADS * HEAD), F32),
        ),
        in_specs=[vmem] * 6 + [smem, vmem],
        out_specs=(vmem, vmem, vmem),
        scratch_shapes=[
            pltpu.VMEM((8, TOK), F32),
            pltpu.VMEM((2, 8, 8, TOK), F32),
            pltpu.VMEM((8, 8, TOK), F32),
            pltpu.VMEM((8, 8, TOK), F32),
            pltpu.VMEM((8, TOK, 2 * HEAD), BF16),
            pltpu.VMEM((8, TOK, 2 * HEAD), BF16),
            pltpu.VMEM((2, 2, 8, TOK, HEAD), BF16),
            pltpu.VMEM((D, TOK), BF16),
            pltpu.VMEM((8, XROWS, TOK), BF16),
            pltpu.VMEM((HEAD, 512), BF16),
            pltpu.VMEM((8, HEAD, 2 * TOK), F32),
            pltpu.VMEM((2, 2, 512, HEAD), F32),
            pltpu.VMEM((2, 2, 512, HEAD), BF16),
            pltpu.VMEM((2, 2, 512, HEAD), BF16),
            pltpu.VMEM((4, 1024, HEAD), BF16),
            pltpu.VMEM((8, TOK, 2 * HEAD), BF16),
            pltpu.VMEM((8, TOK, HEAD), BF16),
            pltpu.VMEM((4, 4, QROWS, HEAD), BF16),
            pltpu.VMEM((4, 3, QROWS, HEAD), BF16),
            pltpu.VMEM((4, 2, HALF, HEAD), BF16),
            pltpu.VMEM((8, HALF, HEAD), BF16),
            pltpu.VMEM((HALF, HEAD), BF16),
            pltpu.VMEM((8, 2, HALF, HEAD), BF16),
            dma((6, 7)), dma((6, 7)), dma((6,)),
            dma((2, 8)), dma((2, 8)),
            dma((3,)), dma((3,)), dma,
            dma((4,)), dma((4,)),
            dma((2,)), dma((2,)),
            dma((2, 3)), dma((2, 3)),
            dma((2, 7)), dma((2, 7)), dma((2,)),
            dma((4, 3)), dma((4, 3)),
            dma((4, 2)), dma((8,)),
            dma((16,)), dma((8, 2)),
        ],
        compiler_params=pltpu.CompilerParams(
            collective_id=0, has_side_effects=True, vmem_limit_bytes=50 * 2**20
        ),
    )(
        query_rows[0], output_grad[0], attn_output[0], key_rows[0], value_rows[0],
        log_norm[0], slab_order, normed_input[0],
    )
    return grad_query[None], grad_key[None], weight


def solution(mesh):
    placed = (
        P("batch", "seq", None),
        P("batch", "seq", None),
        P("batch", "seq", None),
        P("batch", "seq", None),
        P("batch", "seq", None),
        P("batch", None, "seq"),
        P("batch", "seq"),
        P("batch", "seq", None),
    )
    return jax.shard_map(
        local,
        mesh=mesh,
        in_specs=placed,
        out_specs=(P("batch", "seq", None), P("batch", "seq", None), P("seq", None)),
        check_vma=False,
    )
```

```python
import functools

import jax
import jax.numpy as jnp
from jax import lax
from jax.experimental import pallas as pl
from jax.experimental.pallas import tpu as pltpu
from jax.sharding import PartitionSpec as P

HEADS = 16
KV_HEADS = 8
HEAD = 128
TOK = 128
D = 4608
XROWS = D // 4
QROWS = D // 16
PIECE = QROWS // 8

SCALE = 144.0 ** (-0.5)
LOG2E = 1.4426950408889634

MESH = pl.DeviceIdType.MESH
F32 = jnp.float32
BF16 = jnp.bfloat16

RELS = ((0, 1), (1, 0), (1, 1), (3, 0), (3, 1), (2, 0), (2, 1))
STEPS = (1, 3, 2)


def dot(a, b):
    return lax.dot_general(a, b, (((1,), (0,)), ((), ())), preferred_element_type=F32)


def dot_nt(a, b):
    return lax.dot_general(a, b, (((1,), (1,)), ((), ())), preferred_element_type=F32)


def kernel(
    q_hbm, do_hbm, o_hbm, k_hbm, v_hbm, ln_hbm, n_hbm, slab_ref,
    gq_ref, gk_ref, w_ref,
    q_ref, do_ref, o_ref, k_ref, v_ref, ln_ref, n_ref, in_s, pos_s, pos_r, aux_s, aux_r, q_r, do_r, kv_r, nt_s, nt_r, kt, dqt, acc, dkv_s, dkv_r,
    dvg, dq_s, dk_s, wy_s, wy_r, wz_s, wz_r, mid, wa_s, wf,
    x_ss, x_rs, x_ls, y_ss, y_rs, n_ss, n_rs, n_ls, p_ss, p_rs, dy_ss, dy_rs, dv_ss, dv_rs,
    g_ss, g_rs, g_ls, wy_ss, wy_rs, wz_ss, wz_rs, wm_ss, wm_rs, wo_ss, wo_rs, wa_ss, wa_rs,
):
    seq = lax.axis_index("seq")
    batch = lax.axis_index("batch")
    x, yh, c = seq // 4, (seq // 2) % 2, seq % 2
    yl, z = batch // 8, batch % 8
    y = 2 * yh + yl

    def device(x_, y_, c_, z_):
        return {"seq": 4 * x_ + 2 * (y_ // 2) + c_, "batch": 8 * (y_ % 2) + z_}

    def along_x(step):
        return (x + step) % 4

    def remote(src, dst, ss, rs, to):
        copy = pltpu.make_async_remote_copy(
            src_ref=src, dst_ref=dst, send_sem=ss, recv_sem=rs,
            device_id=to, device_id_type=MESH,
        )
        copy.start()
        return copy

    def keep(src, dst, sem):
        copy = pltpu.make_async_copy(src, dst, sem)
        copy.start()
        return copy

    g = 2 * x + c
    partner = device(x, (y + 2) % 4, c, z)
    peers = [device(along_x(dx), y, (c + dc) % 2, z) for dx, dc in RELS]
    slots = [2 * along_x(dx) + (c + dc) % 2 for dx, dc in RELS]
    sources = [2 * along_x(4 - dx) + (c + dc) % 2 for dx, dc in RELS]

    staged = [
        keep(source, target, in_s.at[i])
        for i, (source, target) in enumerate((
            (k_hbm, k_ref), (v_hbm, v_ref), (do_hbm, do_ref), (o_hbm, o_ref),
            (ln_hbm, ln_ref), (q_hbm, q_ref), (n_hbm, n_ref),
        ))
    ]
    pos_s[...] = jnp.full((8, TOK), slab_ref[0, 0] * TOK, jnp.int32).astype(F32)

    barrier = pltpu.get_barrier_semaphore()
    for to in peers:
        pl.semaphore_signal(barrier, inc=1, device_id=to, device_id_type=MESH)
    for step in STEPS:
        to = device(x, (y + step) % 4, c, z)
        pl.semaphore_signal(barrier, inc=1, device_id=to, device_id_type=MESH)
    for dyl in range(2):
        for dc in range(2):
            for dz in range(8):
                if dyl + dc + dz > 0:
                    to = device(x, 2 * yh + (yl + dyl) % 2, (c + dc) % 2, (z + dz) % 8)
                    pl.semaphore_signal(barrier, inc=1, device_id=to, device_id_type=MESH)
    pl.semaphore_wait(barrier, 41)

    staged[0].wait()
    staged[1].wait()

    def columns(ref, slot, width):
        return ref.at[:, pl.ds(pl.multiple_of(slot * width, width), width)]

    first, own_first = [], [
        keep(columns(k_ref, g, HEAD), kv_r.at[0, 0, g], x_ls.at[0]),
        keep(columns(v_ref, g, HEAD), kv_r.at[0, 1, g], x_ls.at[1]),
        keep(pos_s, pos_r.at[0, g], x_ls.at[2]),
    ]
    for r, to in enumerate(peers):
        first.append([
            remote(columns(k_ref, slots[r], HEAD), kv_r.at[0, 0, g], x_ss.at[0, r], x_rs.at[0, r], to),
            remote(columns(v_ref, slots[r], HEAD), kv_r.at[0, 1, g], x_ss.at[1, r], x_rs.at[1, r], to),
            remote(pos_s, pos_r.at[0, g], x_ss.at[2, r], x_rs.at[2, r], to),
        ])

    for copy in staged[2:6]:
        copy.wait()
    lane = lax.broadcasted_iota(jnp.int32, (1, TOK), 1).astype(F32)
    here = pos_s[0:1, :] + lane

    def delta_of(h, carry):
        rows = []
        for e in range(2):
            at = pl.ds(pl.multiple_of((2 * h + e) * HEAD, HEAD), HEAD)
            both = do_ref[:, at].astype(F32) * o_ref[:, at].astype(F32)
            rows.append(jnp.sum(both.T, axis=0, keepdims=True))
        norms = ln_ref[pl.ds(2 * h, 2), :] * LOG2E
        aux_s[h] = jnp.concatenate([norms, *rows, here, jnp.zeros((3, TOK), F32)], axis=0)
        return carry

    lax.fori_loop(0, KV_HEADS, delta_of, 0)

    second, own_second = [], [
        keep(aux_s.at[g], aux_r.at[0], x_ls.at[3]),
        keep(columns(q_ref, g, 2 * HEAD), q_r.at[0], x_ls.at[4]),
        keep(columns(do_ref, g, 2 * HEAD), do_r.at[0], x_ls.at[5]),
    ]
    for r, to in enumerate(peers):
        second.append([
            remote(columns(q_ref, slots[r], 2 * HEAD), q_r.at[r + 1], x_ss.at[4, r], x_rs.at[4, r], to),
            remote(columns(do_ref, slots[r], 2 * HEAD), do_r.at[r + 1], x_ss.at[5, r], x_rs.at[5, r], to),
            remote(aux_s.at[slots[r]], aux_r.at[r + 1], x_ss.at[3, r], x_rs.at[3, r], to),
        ])

    passed = []

    def pass_on(slot, r):
        passed.append(remote(kv_r.at[0, :, slot], kv_r.at[1, :, slot], y_ss.at[0, r], y_rs.at[0, r], partner))
        passed.append(remote(pos_r.at[0, slot], pos_r.at[1, slot], y_ss.at[1, r], y_rs.at[1, r], partner))

    for copy in own_first:
        copy.wait()
    pass_on(g, 7)

    staged[6].wait()

    def turn(b, carry):
        at = pl.ds(pl.multiple_of(b * 128, 128), 128)
        nt_s[at, :] = n_ref[:, at].astype(F32).T.astype(BF16)
        return carry

    lax.fori_loop(0, D // 128, turn, 0)

    for r in range(7):
        for copy in first[r]:
            copy.wait_recv()
        pass_on(sources[r], r)

    def x_rows(step):
        return nt_s.at[pl.ds(pl.multiple_of(along_x(step) * XROWS, 128), XROWS), :]

    inputs = [keep(x_rows(0), nt_r.at[g], n_ls)]
    for i, step in enumerate(STEPS):
        inputs.append(
            remote(x_rows(step), nt_r.at[g], n_ss.at[i], n_rs.at[i], device(along_x(step), y, c, z))
        )

    key_at = lax.broadcasted_iota(jnp.int32, (TOK, TOK), 0).astype(F32)

    def start(half, b):
        for k in range(4):
            kt[half, b, :, 128 * k : 128 * k + 128] = kv_r[half, 0, 4 * b + k].astype(F32).T.astype(BF16)
        acc[half, b] = jnp.zeros((2, 512, HEAD), F32)

    def block(half, b, low, high, fresh=False):
        def step(j, carry):
            queries = jnp.concatenate([q_r[j, :, :HEAD], q_r[j, :, HEAD:]], axis=0)
            grads = jnp.concatenate([do_r[j, :, :HEAD], do_r[j, :, HEAD:]], axis=0)
            aux = aux_r[j]
            norms = jnp.concatenate([aux[0:1], aux[1:2]], axis=1)
            delta = jnp.concatenate([aux[2:3], aux[3:4]], axis=1)
            query_pos = aux[4:5]
            keys = kv_r[half, 0, 4 * b : 4 * b + 4].reshape(512, HEAD)
            values = kv_r[half, 1, 4 * b : 4 * b + 4].reshape(512, HEAD)
            scores = dot_nt(keys, queries)
            dprob = dot_nt(values, grads)
            probs, dscores = [], []
            for k in range(4):
                rows = slice(128 * k, 128 * k + 128)
                ahead = query_pos - pos_r[half, 4 * b + k][0:1]
                allowed = ahead >= key_at
                prob = jnp.exp2(scores[rows] * (SCALE * LOG2E) - norms)
                prob = jnp.concatenate(
                    [jnp.where(allowed, prob[:, :128], 0.0), jnp.where(allowed, prob[:, 128:], 0.0)], axis=1
                )
                probs.append(prob.astype(BF16))
                dscores.append((prob * (dprob[rows] - delta)).astype(BF16))
            prob = jnp.concatenate(probs, axis=0)
            dscore = jnp.concatenate(dscores, axis=0)
            acc[half, b, 0] += dot(dscore, queries)
            acc[half, b, 1] += dot(prob, grads)
            term = dot(kt[half, b], dscore)
            if fresh:
                dqt[j] = term
            else:
                dqt[j] += term
            return carry

        lax.fori_loop(low, high, step, 0, unroll=2)

    across = {}

    def send_across(b, part):
        dkv_s[b, part] = acc[1, b, part].astype(BF16)
        across[b, part] = remote(
            dkv_s.at[b, part], dkv_r.at[b, part], dy_ss.at[b, part], dy_rs.at[b, part], partner
        )

    values_out = {}

    def finish_values(b):
        across[b, 1].wait_recv()
        dvg[0, 512 * b : 512 * b + 512] = (acc[0, b, 1] + dkv_r[b, 1].astype(F32)).astype(BF16)

    def send_values(b, i):
        rows = slice(512 * b, 512 * b + 512)
        values_out[b, i] = remote(
            dvg.at[0, rows], dvg.at[i + 1, rows], dv_ss.at[b, i], dv_rs.at[b, i],
            device(along_x(STEPS[i]), y, c, z),
        )

    def finish_keys(b):
        across[b, 0].wait_recv()
        keys_done = (SCALE * (acc[0, b, 0] + dkv_r[b, 0].astype(F32))).astype(BF16)
        dk_s[4 * b : 4 * b + 4] = keys_done.reshape(4, 128, HEAD)

    other = device(x, y, (c + 1) % 2, z)
    shared = []

    def share(i, step):
        if i == 0:
            inputs[0].wait()
        else:
            inputs[i].wait_recv()
        j = 2 * along_x(step) + c
        shared.append(remote(nt_r.at[j], nt_r.at[j], p_ss.at[i], p_rs.at[i], other))

    def arrived(low, high):
        for r in range(low, high):
            for copy in second[r]:
                copy.wait_recv()

    start(0, 0)
    for copy in own_second:
        copy.wait()
    arrived(0, 5)
    block(0, 0, 0, 6, fresh=True)
    for copy in passed:
        copy.wait_recv()
    start(1, 0)
    block(1, 0, 0, 6)
    arrived(5, 7)
    block(1, 0, 6, 8, fresh=True)
    send_across(0, 1)
    start(1, 1)
    block(1, 1, 0, 8)
    send_across(1, 1)
    send_across(0, 0)
    send_across(1, 0)
    share(0, 0)
    block(0, 0, 6, 8)
    finish_values(0)
    send_values(0, 0)
    send_values(0, 1)
    start(0, 1)
    block(0, 1, 0, 8)
    finish_values(1)
    send_values(1, 0)
    send_values(1, 1)
    send_values(0, 2)
    send_values(1, 2)
    share(1, 3)
    share(2, 1)
    share(3, 2)

    def queries_done(j, carry):
        dq_s[j] = jnp.concatenate(
            [(SCALE * dqt[j, :, :128]).T, (SCALE * dqt[j, :, 128:]).T], axis=1
        ).astype(BF16)
        return carry

    lax.fori_loop(0, 8, queries_done, 0)

    for copy in shared:
        copy.wait_recv()

    back = []

    def send_back():
        finish_keys(0)
        finish_keys(1)
        back.extend([
            keep(dk_s.at[g], columns(gk_ref, g, HEAD), g_ls.at[0]),
            keep(dq_s.at[0], columns(gq_ref, g, 2 * HEAD), g_ls.at[1]),
        ])
        for r, (dx, dc) in enumerate(RELS):
            to = device(along_x(4 - dx), y, (c + dc) % 2, z)
            back.append(remote(dk_s.at[sources[r]], columns(gk_ref, g, HEAD), g_ss.at[0, r], g_rs.at[0, r], to))
            back.append(remote(dq_s.at[r + 1], columns(gq_ref, g, 2 * HEAD), g_ss.at[1, r], g_rs.at[1, r], to))

    over_y = []

    def multiply(i):
        if i > 0:
            values_out[0, i - 1].wait_recv()
            values_out[1, i - 1].wait_recv()

        def quarter(t, carry):
            at = pl.ds(pl.multiple_of(t * QROWS, 32), QROWS)
            total = None
            for j in range(4):
                left = jnp.concatenate([nt_r[2 * j, at, :], nt_r[2 * j + 1, at, :]], axis=1)
                term = dot(left, dvg[i, 256 * j : 256 * j + 256])
                total = term if total is None else total + term
            wy_s[i, t] = total.astype(BF16)
            return carry

        lax.fori_loop(0, 4, quarter, 0)
        over_y.append([
            remote(
                wy_s.at[i, (y + step) % 4], wy_r.at[i, k], wy_ss.at[i, k], wy_rs.at[i, k],
                device(x, (y + step) % 4, c, z),
            )
            for k, step in enumerate(STEPS)
        ])

    over_z = []

    def reduce_y(i):
        total = wy_s[i, y].astype(F32)
        for k in range(3):
            over_y[i][k].wait_recv()
            total = total + wy_r[i, k].astype(F32)
        for k in range(8):
            wz_s[i, k] = total[PIECE * k : PIECE * k + PIECE].astype(BF16)
        over_z.append([
            remote(
                wz_s.at[i, (z + k) % 8], wz_r.at[i, k - 1], wz_ss.at[i, k - 1], wz_rs.at[i, k - 1],
                device(x, y, c, (z + k) % 8),
            )
            for k in (4, 3, 5, 2, 6, 1, 7)
        ])

    def column_block(i, core):
        return 2 * along_x((0, 3, 1, 2)[i]) + core

    def sum_z(i):
        total = wz_s[i, z].astype(F32)
        for copy in over_z[i]:
            copy.wait_recv()
        for k in range(7):
            total = total + wz_r[i, k].astype(F32)
        return total.astype(BF16)

    def w_copy(t):
        dyl, dz = t // 8, t % 8
        return pltpu.make_async_remote_copy(
            src_ref=wa_s, dst_ref=wf.at[column_block(3, c), z], send_sem=wa_ss.at[t], recv_sem=wa_rs.at[c, z],
            device_id=device(x, 2 * yh + (yl + dyl) % 2, yl, (z + dz) % 8), device_id_type=MESH,
        )

    def last_z():
        wa_s[...] = sum_z(3)
        for t in (12, 4, 11, 3, 13, 5, 10, 2, 14, 6, 9, 1, 15, 7, 8):
            w_copy(t).start()
        pl.when(c != yl)(lambda: w_copy(0).start())
        pl.when(c == yl)(
            lambda: pltpu.make_async_copy(wa_s, wf.at[column_block(3, c), z], wa_rs.at[c, z]).start()
        )

    gathered = []

    def reduce_z(i):
        mid[i, z] = sum_z(i)
        gathered.append([
            remote(
                mid.at[i, z], mid.at[i, z], wm_ss.at[i, k - 1], wm_rs.at[i, k - 1],
                device(x, y, c, (z + k) % 8),
            )
            for k in (4, 3, 5, 2, 6, 1, 7)
        ])

    def near_copy(i):
        block = column_block(i, c)
        return pltpu.make_async_remote_copy(
            src_ref=mid.at[i], dst_ref=wf.at[block], send_sem=wo_ss.at[i, 0], recv_sem=wo_rs.at[block],
            device_id=device(x, y, yl, z), device_id_type=MESH,
        )

    handed = []

    def hand_over(i):
        for copy in gathered[i]:
            copy.wait_recv()
        block = column_block(i, c)
        handed.append(
            remote(
                mid.at[i], wf.at[block], wo_ss.at[i, 1], wo_rs.at[block],
                device(x, 2 * yh + (yl + 1) % 2, yl, z),
            )
        )
        pl.when(c != yl)(lambda: near_copy(i).start())
        pl.when(c == yl)(lambda: pltpu.make_async_copy(mid.at[i], wf.at[block], wo_rs.at[block]).start())

    multiply(0)
    send_back()
    multiply(1)
    multiply(2)
    reduce_y(0)
    multiply(3)
    reduce_y(1)
    reduce_z(0)
    reduce_y(2)
    reduce_z(1)
    hand_over(0)
    reduce_y(3)
    reduce_z(2)
    hand_over(1)
    last_z()
    hand_over(2)

    for copy in back:
        if copy is back[0] or copy is back[1]:
            copy.wait()
        else:
            copy.wait_recv()

    for i in range(4):
        for core in range(2):
            block = column_block(i, core)
            at = pl.ds(pl.multiple_of(128 * block, 128), 128)
            if i < 3:
                pltpu.make_async_copy(mid.at[i], wf.at[block], wo_rs.at[block]).wait()
            for k in range(8):
                if i == 3:
                    pltpu.make_async_copy(wa_s, wf.at[block, k], wa_rs.at[core, k]).wait()
                w_ref[PIECE * k : PIECE * k + PIECE, at] = wf[block, k].astype(F32)

    for group in first + second + over_y + over_z + gathered:
        for copy in group:
            copy.wait_send()
    for copy in passed + inputs[1:] + shared + [*across.values(), *values_out.values()] + back[2:] + handed:
        copy.wait_send()
    for t in range(1, 16):
        w_copy(t).wait_send()
    pl.when(c != yl)(lambda: w_copy(0).wait_send())
    for i in range(3):
        pl.when(c != yl)(lambda: near_copy(i).wait_send())


def local(
    query_rows, key_rows, value_rows, attn_output, output_grad, log_norm, slab_order, normed_input
):
    vmem = pl.BlockSpec(memory_space=pltpu.VMEM)
    smem = pl.BlockSpec(memory_space=pltpu.SMEM)
    dma = pltpu.SemaphoreType.DMA
    grad_query, grad_key, weight = pl.pallas_call(
        kernel,
        name="step",
        out_shape=(
            jax.ShapeDtypeStruct((TOK, HEADS * HEAD), BF16),
            jax.ShapeDtypeStruct((TOK, KV_HEADS * HEAD), BF16),
            jax.ShapeDtypeStruct((QROWS, KV_HEADS * HEAD), F32),
        ),
        in_specs=[pl.BlockSpec(memory_space=pltpu.HBM)] * 7 + [smem],
        out_specs=(vmem, vmem, vmem),
        scratch_shapes=[
            pltpu.VMEM((TOK, HEADS * HEAD), BF16),
            pltpu.VMEM((TOK, HEADS * HEAD), BF16),
            pltpu.VMEM((TOK, HEADS * HEAD), BF16),
            pltpu.VMEM((TOK, KV_HEADS * HEAD), BF16),
            pltpu.VMEM((TOK, KV_HEADS * HEAD), BF16),
            pltpu.VMEM((HEADS, TOK), F32),
            pltpu.VMEM((TOK, D), BF16),
            dma((7,)),
            pltpu.VMEM((8, TOK), F32),
            pltpu.VMEM((2, 8, 8, TOK), F32),
            pltpu.VMEM((8, 8, TOK), F32),
            pltpu.VMEM((8, 8, TOK), F32),
            pltpu.VMEM((8, TOK, 2 * HEAD), BF16),
            pltpu.VMEM((8, TOK, 2 * HEAD), BF16),
            pltpu.VMEM((2, 2, 8, TOK, HEAD), BF16),
            pltpu.VMEM((D, TOK), BF16),
            pltpu.VMEM((8, XROWS, TOK), BF16),
            pltpu.VMEM((2, 2, HEAD, 512), BF16),
            pltpu.VMEM((8, HEAD, 2 * TOK), F32),
            pltpu.VMEM((2, 2, 2, 512, HEAD), F32),
            pltpu.VMEM((2, 2, 512, HEAD), BF16),
            pltpu.VMEM((2, 2, 512, HEAD), BF16),
            pltpu.VMEM((4, 1024, HEAD), BF16),
            pltpu.VMEM((8, TOK, 2 * HEAD), BF16),
            pltpu.VMEM((8, TOK, HEAD), BF16),
            pltpu.VMEM((4, 4, QROWS, HEAD), BF16),
            pltpu.VMEM((4, 3, QROWS, HEAD), BF16),
            pltpu.VMEM((4, 8, PIECE, HEAD), BF16),
            pltpu.VMEM((4, 7, PIECE, HEAD), BF16),
            pltpu.VMEM((3, 8, PIECE, HEAD), BF16),
            pltpu.VMEM((PIECE, HEAD), BF16),
            pltpu.VMEM((8, 8, PIECE, HEAD), BF16),
            dma((6, 7)), dma((6, 7)), dma((6,)),
            dma((2, 8)), dma((2, 8)),
            dma((3,)), dma((3,)), dma,
            dma((4,)), dma((4,)),
            dma((2, 2)), dma((2, 2)),
            dma((2, 3)), dma((2, 3)),
            dma((2, 7)), dma((2, 7)), dma((2,)),
            dma((4, 3)), dma((4, 3)),
            dma((4, 7)), dma((4, 7)),
            dma((3, 7)), dma((3, 7)), dma((3, 2)), dma((8,)),
            dma((16,)), dma((2, 8)),
        ],
        compiler_params=pltpu.CompilerParams(
            collective_id=0, has_side_effects=True, vmem_limit_bytes=44 * 2**20
        ),
    )(
        *(
            pltpu.with_memory_space_constraint(part[0], pltpu.HBM)
            for part in (query_rows, output_grad, attn_output, key_rows, value_rows, log_norm, normed_input)
        ),
        slab_order,
    )
    return grad_query[None], grad_key[None], weight


def solution(mesh):
    placed = (
        P("batch", "seq", None),
        P("batch", "seq", None),
        P("batch", "seq", None),
        P("batch", "seq", None),
        P("batch", "seq", None),
        P("batch", None, "seq"),
        P("batch", "seq"),
        P("batch", "seq", None),
    )
    return jax.shard_map(
        local,
        mesh=mesh,
        in_specs=placed,
        out_specs=(P("batch", "seq", None), P("batch", "seq", None), P("seq", None)),
        check_vma=False,
    )
```

```python
import functools

import jax
import jax.numpy as jnp
from jax import lax
from jax.experimental import pallas as pl
from jax.experimental.pallas import tpu as pltpu
from jax.sharding import PartitionSpec as P

HEADS = 16
KV_HEADS = 8
HEAD = 128
TOK = 128
D = 4608
XROWS = D // 4
QROWS = D // 16
PIECE = QROWS // 8

SCALE = 144.0 ** (-0.5)
LOG2E = 1.4426950408889634

MESH = pl.DeviceIdType.MESH
F32 = jnp.float32
BF16 = jnp.bfloat16

RELS = ((0, 1), (1, 0), (1, 1), (3, 0), (3, 1), (2, 0), (2, 1))
STEPS = (1, 3, 2)


def dot(a, b):
    return lax.dot_general(a, b, (((1,), (0,)), ((), ())), preferred_element_type=F32)


def dot_nt(a, b):
    return lax.dot_general(a, b, (((1,), (1,)), ((), ())), preferred_element_type=F32)


def kernel(
    q_hbm, do_hbm, o_hbm, k_hbm, v_hbm, ln_hbm, n_hbm, slab_ref,
    gq_ref, gk_ref, w_ref,
    q_ref, do_ref, o_ref, k_ref, v_ref, ln_ref, n_ref, in_s, pos_s, pos_r, aux_s, aux_r, q_r, do_r, kv_r, nt_s, nt_r, kt, dqt, acc, dkv_s, dkv_r,
    dvg, dq_s, dk_s, wy_s, wy_r, wz_s, wz_r, mid, wa_s, wf,
    x_ss, x_rs, x_ls, y_ss, y_rs, n_ss, n_rs, n_ls, p_ss, p_rs, dy_ss, dy_rs, dv_ss, dv_rs,
    g_ss, g_rs, g_ls, wy_ss, wy_rs, wz_ss, wz_rs, wm_ss, wm_rs, wo_ss, wo_rs, wa_ss, wa_rs,
):
    seq = lax.axis_index("seq")
    batch = lax.axis_index("batch")
    x, yh, c = seq // 4, (seq // 2) % 2, seq % 2
    yl, z = batch // 8, batch % 8
    y = 2 * yh + yl

    def device(x_, y_, c_, z_):
        return {"seq": 4 * x_ + 2 * (y_ // 2) + c_, "batch": 8 * (y_ % 2) + z_}

    def along_x(step):
        return (x + step) % 4

    def remote(src, dst, ss, rs, to):
        copy = pltpu.make_async_remote_copy(
            src_ref=src, dst_ref=dst, send_sem=ss, recv_sem=rs,
            device_id=to, device_id_type=MESH,
        )
        copy.start()
        return copy

    def keep(src, dst, sem):
        copy = pltpu.make_async_copy(src, dst, sem)
        copy.start()
        return copy

    g = 2 * x + c
    partner = device(x, (y + 2) % 4, c, z)
    peers = [device(along_x(dx), y, (c + dc) % 2, z) for dx, dc in RELS]
    slots = [2 * along_x(dx) + (c + dc) % 2 for dx, dc in RELS]
    sources = [2 * along_x(4 - dx) + (c + dc) % 2 for dx, dc in RELS]

    staged = [
        keep(source, target, in_s.at[i])
        for i, (source, target) in enumerate((
            (k_hbm, k_ref), (v_hbm, v_ref), (do_hbm, do_ref), (o_hbm, o_ref),
            (ln_hbm, ln_ref), (q_hbm, q_ref), (n_hbm, n_ref),
        ))
    ]
    pos_s[...] = jnp.full((8, TOK), slab_ref[0, 0] * TOK, jnp.int32).astype(F32)

    barrier = pltpu.get_barrier_semaphore()
    for to in peers:
        pl.semaphore_signal(barrier, inc=1, device_id=to, device_id_type=MESH)
    for step in STEPS:
        to = device(x, (y + step) % 4, c, z)
        pl.semaphore_signal(barrier, inc=1, device_id=to, device_id_type=MESH)
    for dyl in range(2):
        for dc in range(2):
            for dz in range(8):
                if dyl + dc + dz > 0:
                    to = device(x, 2 * yh + (yl + dyl) % 2, (c + dc) % 2, (z + dz) % 8)
                    pl.semaphore_signal(barrier, inc=1, device_id=to, device_id_type=MESH)
    pl.semaphore_wait(barrier, 41)

    staged[0].wait()
    staged[1].wait()

    def columns(ref, slot, width):
        return ref.at[:, pl.ds(pl.multiple_of(slot * width, width), width)]

    first, own_first = [], [
        keep(columns(k_ref, g, HEAD), kv_r.at[0, 0, g], x_ls.at[0]),
        keep(columns(v_ref, g, HEAD), kv_r.at[0, 1, g], x_ls.at[1]),
        keep(pos_s, pos_r.at[0, g], x_ls.at[2]),
    ]
    for r, to in enumerate(peers):
        first.append([
            remote(columns(k_ref, slots[r], HEAD), kv_r.at[0, 0, g], x_ss.at[0, r], x_rs.at[0, r], to),
            remote(columns(v_ref, slots[r], HEAD), kv_r.at[0, 1, g], x_ss.at[1, r], x_rs.at[1, r], to),
            remote(pos_s, pos_r.at[0, g], x_ss.at[2, r], x_rs.at[2, r], to),
        ])

    for copy in staged[2:6]:
        copy.wait()
    lane = lax.broadcasted_iota(jnp.int32, (1, TOK), 1).astype(F32)
    here = pos_s[0:1, :] + lane

    def delta_of(h, carry):
        rows = []
        for e in range(2):
            at = pl.ds(pl.multiple_of((2 * h + e) * HEAD, HEAD), HEAD)
            both = do_ref[:, at].astype(F32) * o_ref[:, at].astype(F32)
            rows.append(jnp.sum(both.T, axis=0, keepdims=True))
        norms = ln_ref[pl.ds(2 * h, 2), :] * LOG2E
        aux_s[h] = jnp.concatenate([norms, *rows, here, jnp.zeros((3, TOK), F32)], axis=0)
        return carry

    lax.fori_loop(0, KV_HEADS, delta_of, 0)

    second, own_second = [], [
        keep(aux_s.at[g], aux_r.at[0], x_ls.at[3]),
        keep(columns(q_ref, g, 2 * HEAD), q_r.at[0], x_ls.at[4]),
        keep(columns(do_ref, g, 2 * HEAD), do_r.at[0], x_ls.at[5]),
    ]
    for r, to in enumerate(peers):
        second.append([
            remote(columns(q_ref, slots[r], 2 * HEAD), q_r.at[r + 1], x_ss.at[4, r], x_rs.at[4, r], to),
            remote(columns(do_ref, slots[r], 2 * HEAD), do_r.at[r + 1], x_ss.at[5, r], x_rs.at[5, r], to),
            remote(aux_s.at[slots[r]], aux_r.at[r + 1], x_ss.at[3, r], x_rs.at[3, r], to),
        ])

    passed = []

    def pass_on(slot, r):
        passed.append(remote(kv_r.at[0, :, slot], kv_r.at[1, :, slot], y_ss.at[0, r], y_rs.at[0, r], partner))
        passed.append(remote(pos_r.at[0, slot], pos_r.at[1, slot], y_ss.at[1, r], y_rs.at[1, r], partner))

    for copy in own_first:
        copy.wait()
    pass_on(g, 7)

    for r in range(7):
        for copy in first[r]:
            copy.wait_recv()
        pass_on(sources[r], r)

    staged[6].wait()

    def turn(b, carry):
        at = pl.ds(pl.multiple_of(b * 128, 128), 128)
        nt_s[at, :] = n_ref[:, at].astype(F32).T.astype(BF16)
        return carry

    lax.fori_loop(0, D // 128, turn, 0)

    def x_rows(step):
        return nt_s.at[pl.ds(pl.multiple_of(along_x(step) * XROWS, 128), XROWS), :]

    inputs = [keep(x_rows(0), nt_r.at[g], n_ls)]
    for i, step in enumerate(STEPS):
        inputs.append(
            remote(x_rows(step), nt_r.at[g], n_ss.at[i], n_rs.at[i], device(along_x(step), y, c, z))
        )

    key_at = lax.broadcasted_iota(jnp.int32, (TOK, TOK), 0).astype(F32)

    def start(half, b):
        for k in range(4):
            kt[half, b, :, 128 * k : 128 * k + 128] = kv_r[half, 0, 4 * b + k].astype(F32).T.astype(BF16)
        acc[half, b] = jnp.zeros((2, 512, HEAD), F32)

    def block(half, b, low, high, fresh=False):
        def step(j, carry):
            queries = jnp.concatenate([q_r[j, :, :HEAD], q_r[j, :, HEAD:]], axis=0)
            grads = jnp.concatenate([do_r[j, :, :HEAD], do_r[j, :, HEAD:]], axis=0)
            aux = aux_r[j]
            norms = jnp.concatenate([aux[0:1], aux[1:2]], axis=1)
            delta = jnp.concatenate([aux[2:3], aux[3:4]], axis=1)
            query_pos = aux[4:5]
            keys = kv_r[half, 0, 4 * b : 4 * b + 4].reshape(512, HEAD)
            values = kv_r[half, 1, 4 * b : 4 * b + 4].reshape(512, HEAD)
            scores = dot_nt(keys, queries)
            dprob = dot_nt(values, grads)
            probs, dscores = [], []
            for k in range(4):
                rows = slice(128 * k, 128 * k + 128)
                ahead = query_pos - pos_r[half, 4 * b + k][0:1]
                allowed = ahead >= key_at
                prob = jnp.exp2(scores[rows] * (SCALE * LOG2E) - norms)
                prob = jnp.concatenate(
                    [jnp.where(allowed, prob[:, :128], 0.0), jnp.where(allowed, prob[:, 128:], 0.0)], axis=1
                )
                probs.append(prob.astype(BF16))
                dscores.append((prob * (dprob[rows] - delta)).astype(BF16))
            prob = jnp.concatenate(probs, axis=0)
            dscore = jnp.concatenate(dscores, axis=0)
            acc[half, b, 0] += dot(dscore, queries)
            acc[half, b, 1] += dot(prob, grads)
            term = dot(kt[half, b], dscore)
            if fresh:
                dqt[j] = term
            else:
                dqt[j] += term
            return carry

        lax.fori_loop(low, high, step, 0, unroll=2)

    across = {}

    def send_across(b, part):
        dkv_s[b, part] = acc[1, b, part].astype(BF16)
        across[b, part] = remote(
            dkv_s.at[b, part], dkv_r.at[b, part], dy_ss.at[b, part], dy_rs.at[b, part], partner
        )

    values_out = {}

    def finish_values(b):
        across[b, 1].wait_recv()
        dvg[0, 512 * b : 512 * b + 512] = (acc[0, b, 1] + dkv_r[b, 1].astype(F32)).astype(BF16)

    def send_values(b, i):
        rows = slice(512 * b, 512 * b + 512)
        values_out[b, i] = remote(
            dvg.at[0, rows], dvg.at[i + 1, rows], dv_ss.at[b, i], dv_rs.at[b, i],
            device(along_x(STEPS[i]), y, c, z),
        )

    def finish_keys(b):
        across[b, 0].wait_recv()
        keys_done = (SCALE * (acc[0, b, 0] + dkv_r[b, 0].astype(F32))).astype(BF16)
        dk_s[4 * b : 4 * b + 4] = keys_done.reshape(4, 128, HEAD)

    other = device(x, y, (c + 1) % 2, z)
    shared = []

    def share(i, step):
        if i == 0:
            inputs[0].wait()
        else:
            inputs[i].wait_recv()
        j = 2 * along_x(step) + c
        shared.append(remote(nt_r.at[j], nt_r.at[j], p_ss.at[i], p_rs.at[i], other))

    def arrived(low, high):
        for r in range(low, high):
            for copy in second[r]:
                copy.wait_recv()

    start(0, 0)
    for copy in own_second:
        copy.wait()
    arrived(0, 5)
    block(0, 0, 0, 6, fresh=True)
    for copy in passed:
        copy.wait_recv()
    start(1, 0)
    block(1, 0, 0, 6)
    arrived(5, 7)
    block(1, 0, 6, 8, fresh=True)
    send_across(0, 1)
    start(1, 1)
    block(1, 1, 0, 8)
    send_across(1, 1)
    send_across(0, 0)
    send_across(1, 0)
    share(0, 0)
    block(0, 0, 6, 8)
    finish_values(0)
    send_values(0, 0)
    send_values(0, 1)
    start(0, 1)
    block(0, 1, 0, 8)
    finish_values(1)
    send_values(1, 0)
    send_values(1, 1)
    send_values(0, 2)
    send_values(1, 2)
    share(1, 3)
    share(2, 1)
    share(3, 2)

    def queries_done(j, carry):
        dq_s[j] = jnp.concatenate(
            [(SCALE * dqt[j, :, :128]).T, (SCALE * dqt[j, :, 128:]).T], axis=1
        ).astype(BF16)
        return carry

    lax.fori_loop(0, 8, queries_done, 0)

    for copy in shared:
        copy.wait_recv()

    back = []

    def send_back():
        finish_keys(0)
        finish_keys(1)
        back.extend([
            keep(dk_s.at[g], columns(gk_ref, g, HEAD), g_ls.at[0]),
            keep(dq_s.at[0], columns(gq_ref, g, 2 * HEAD), g_ls.at[1]),
        ])
        for r, (dx, dc) in enumerate(RELS):
            to = device(along_x(4 - dx), y, (c + dc) % 2, z)
            back.append(remote(dk_s.at[sources[r]], columns(gk_ref, g, HEAD), g_ss.at[0, r], g_rs.at[0, r], to))
            back.append(remote(dq_s.at[r + 1], columns(gq_ref, g, 2 * HEAD), g_ss.at[1, r], g_rs.at[1, r], to))

    over_y = []

    def multiply(i):
        if i > 0:
            values_out[0, i - 1].wait_recv()
            values_out[1, i - 1].wait_recv()

        def quarter(t):
            at = pl.ds(pl.multiple_of(t * QROWS, 32), QROWS)
            total = None
            for j in range(4):
                left = jnp.concatenate([nt_r[2 * j, at, :], nt_r[2 * j + 1, at, :]], axis=1)
                term = dot(left, dvg[i, 256 * j : 256 * j + 256])
                total = term if total is None else total + term
            wy_s[i, t] = total.astype(BF16)

        over_y.append([])
        for k, step in enumerate((2, 1, 3)):
            t = (y + step) % 4
            quarter(t)
            over_y[i].append(
                remote(wy_s.at[i, t], wy_r.at[i, k], wy_ss.at[i, k], wy_rs.at[i, k], device(x, t, c, z))
            )
        quarter(y)

    over_z = []

    def reduce_y(i):
        total = wy_s[i, y].astype(F32)
        for k in range(3):
            over_y[i][k].wait_recv()
            total = total + wy_r[i, k].astype(F32)
        for k in range(8):
            wz_s[i, k] = total[PIECE * k : PIECE * k + PIECE].astype(BF16)
        over_z.append([
            remote(
                wz_s.at[i, (z + k) % 8], wz_r.at[i, k - 1], wz_ss.at[i, k - 1], wz_rs.at[i, k - 1],
                device(x, y, c, (z + k) % 8),
            )
            for k in (4, 3, 5, 2, 6, 1, 7)
        ])

    def column_block(i, core):
        return 2 * along_x((0, 3, 1, 2)[i]) + core

    def sum_z(i):
        total = wz_s[i, z].astype(F32)
        for copy in over_z[i]:
            copy.wait_recv()
        for k in range(7):
            total = total + wz_r[i, k].astype(F32)
        return total.astype(BF16)

    def w_copy(t):
        dyl, dz = t // 8, t % 8
        return pltpu.make_async_remote_copy(
            src_ref=wa_s, dst_ref=wf.at[column_block(3, c), z], send_sem=wa_ss.at[t], recv_sem=wa_rs.at[c, z],
            device_id=device(x, 2 * yh + (yl + dyl) % 2, yl, (z + dz) % 8), device_id_type=MESH,
        )

    def last_z():
        wa_s[...] = sum_z(3)
        for t in (12, 4, 11, 3, 13, 5, 10, 2, 14, 6, 9, 1, 15, 7, 8):
            w_copy(t).start()
        pl.when(c != yl)(lambda: w_copy(0).start())
        pl.when(c == yl)(
            lambda: pltpu.make_async_copy(wa_s, wf.at[column_block(3, c), z], wa_rs.at[c, z]).start()
        )

    gathered = []

    def reduce_z(i):
        mid[i, z] = sum_z(i)
        gathered.append([
            remote(
                mid.at[i, z], mid.at[i, z], wm_ss.at[i, k - 1], wm_rs.at[i, k - 1],
                device(x, y, c, (z + k) % 8),
            )
            for k in (4, 3, 5, 2, 6, 1, 7)
        ])

    def near_copy(i):
        block = column_block(i, c)
        return pltpu.make_async_remote_copy(
            src_ref=mid.at[i], dst_ref=wf.at[block], send_sem=wo_ss.at[i, 0], recv_sem=wo_rs.at[block],
            device_id=device(x, y, yl, z), device_id_type=MESH,
        )

    handed = []

    def hand_over(i):
        for copy in gathered[i]:
            copy.wait_recv()
        block = column_block(i, c)
        handed.append(
            remote(
                mid.at[i], wf.at[block], wo_ss.at[i, 1], wo_rs.at[block],
                device(x, 2 * yh + (yl + 1) % 2, yl, z),
            )
        )
        pl.when(c != yl)(lambda: near_copy(i).start())
        pl.when(c == yl)(lambda: pltpu.make_async_copy(mid.at[i], wf.at[block], wo_rs.at[block]).start())

    multiply(0)
    multiply(1)
    multiply(2)
    reduce_y(0)
    multiply(3)
    send_back()
    reduce_y(1)
    reduce_z(0)
    reduce_y(2)
    reduce_y(3)
    reduce_z(1)
    hand_over(0)
    reduce_z(2)
    last_z()
    hand_over(1)
    hand_over(2)

    for copy in back:
        if copy is back[0] or copy is back[1]:
            copy.wait()
        else:
            copy.wait_recv()

    for i in range(4):
        for core in range(2):
            block = column_block(i, core)
            at = pl.ds(pl.multiple_of(128 * block, 128), 128)
            if i < 3:
                pltpu.make_async_copy(mid.at[i], wf.at[block], wo_rs.at[block]).wait()
            for k in range(8):
                if i == 3:
                    pltpu.make_async_copy(wa_s, wf.at[block, k], wa_rs.at[core, k]).wait()
                w_ref[PIECE * k : PIECE * k + PIECE, at] = wf[block, k].astype(F32)

    for group in first + second + over_y + over_z + gathered:
        for copy in group:
            copy.wait_send()
    for copy in passed + inputs[1:] + shared + [*across.values(), *values_out.values()] + back[2:] + handed:
        copy.wait_send()
    for t in range(1, 16):
        w_copy(t).wait_send()
    pl.when(c != yl)(lambda: w_copy(0).wait_send())
    for i in range(3):
        pl.when(c != yl)(lambda: near_copy(i).wait_send())


def write(gq_ref, gk_ref, w_ref, gq_hbm, gk_hbm, w_hbm, sems):
    copies = [
        pltpu.make_async_copy(source, target, sems.at[i])
        for i, (source, target) in enumerate(((w_ref, w_hbm), (gq_ref, gq_hbm), (gk_ref, gk_hbm)))
    ]
    for copy in copies:
        copy.start()
    for copy in copies:
        copy.wait()


def local(
    query_rows, key_rows, value_rows, attn_output, output_grad, log_norm, slab_order, normed_input
):
    vmem = pl.BlockSpec(memory_space=pltpu.VMEM)
    smem = pl.BlockSpec(memory_space=pltpu.SMEM)
    dma = pltpu.SemaphoreType.DMA
    shapes = (
        jax.ShapeDtypeStruct((TOK, HEADS * HEAD), BF16),
        jax.ShapeDtypeStruct((TOK, KV_HEADS * HEAD), BF16),
        jax.ShapeDtypeStruct((QROWS, KV_HEADS * HEAD), F32),
    )
    results = pl.pallas_call(
        kernel,
        name="step",
        out_shape=shapes,
        in_specs=[pl.BlockSpec(memory_space=pltpu.HBM)] * 7 + [smem],
        out_specs=(vmem, vmem, vmem),
        scratch_shapes=[
            pltpu.VMEM((TOK, HEADS * HEAD), BF16),
            pltpu.VMEM((TOK, HEADS * HEAD), BF16),
            pltpu.VMEM((TOK, HEADS * HEAD), BF16),
            pltpu.VMEM((TOK, KV_HEADS * HEAD), BF16),
            pltpu.VMEM((TOK, KV_HEADS * HEAD), BF16),
            pltpu.VMEM((HEADS, TOK), F32),
            pltpu.VMEM((TOK, D), BF16),
            dma((7,)),
            pltpu.VMEM((8, TOK), F32),
            pltpu.VMEM((2, 8, 8, TOK), F32),
            pltpu.VMEM((8, 8, TOK), F32),
            pltpu.VMEM((8, 8, TOK), F32),
            pltpu.VMEM((8, TOK, 2 * HEAD), BF16),
            pltpu.VMEM((8, TOK, 2 * HEAD), BF16),
            pltpu.VMEM((2, 2, 8, TOK, HEAD), BF16),
            pltpu.VMEM((D, TOK), BF16),
            pltpu.VMEM((8, XROWS, TOK), BF16),
            pltpu.VMEM((2, 2, HEAD, 512), BF16),
            pltpu.VMEM((8, HEAD, 2 * TOK), F32),
            pltpu.VMEM((2, 2, 2, 512, HEAD), F32),
            pltpu.VMEM((2, 2, 512, HEAD), BF16),
            pltpu.VMEM((2, 2, 512, HEAD), BF16),
            pltpu.VMEM((4, 1024, HEAD), BF16),
            pltpu.VMEM((8, TOK, 2 * HEAD), BF16),
            pltpu.VMEM((8, TOK, HEAD), BF16),
            pltpu.VMEM((4, 4, QROWS, HEAD), BF16),
            pltpu.VMEM((4, 3, QROWS, HEAD), BF16),
            pltpu.VMEM((4, 8, PIECE, HEAD), BF16),
            pltpu.VMEM((4, 7, PIECE, HEAD), BF16),
            pltpu.VMEM((3, 8, PIECE, HEAD), BF16),
            pltpu.VMEM((PIECE, HEAD), BF16),
            pltpu.VMEM((8, 8, PIECE, HEAD), BF16),
            dma((6, 7)), dma((6, 7)), dma((6,)),
            dma((2, 8)), dma((2, 8)),
            dma((3,)), dma((3,)), dma,
            dma((4,)), dma((4,)),
            dma((2, 2)), dma((2, 2)),
            dma((2, 3)), dma((2, 3)),
            dma((2, 7)), dma((2, 7)), dma((2,)),
            dma((4, 3)), dma((4, 3)),
            dma((4, 7)), dma((4, 7)),
            dma((3, 7)), dma((3, 7)), dma((3, 2)), dma((8,)),
            dma((16,)), dma((2, 8)),
        ],
        compiler_params=pltpu.CompilerParams(
            collective_id=0, has_side_effects=True, vmem_limit_bytes=44 * 2**20
        ),
    )(
        *(
            pltpu.with_memory_space_constraint(part[0], pltpu.HBM)
            for part in (query_rows, output_grad, attn_output, key_rows, value_rows, log_norm, normed_input)
        ),
        slab_order,
    )
    grad_query, grad_key, weight = pl.pallas_call(
        write,
        name="write",
        out_shape=shapes,
        in_specs=[vmem] * 3,
        out_specs=[pl.BlockSpec(memory_space=pltpu.HBM)] * 3,
        scratch_shapes=[dma((3,))],
        compiler_params=pltpu.CompilerParams(vmem_limit_bytes=2**20),
    )(*results)
    return grad_query[None], grad_key[None], weight


def solution(mesh):
    placed = (
        P("batch", "seq", None),
        P("batch", "seq", None),
        P("batch", "seq", None),
        P("batch", "seq", None),
        P("batch", "seq", None),
        P("batch", None, "seq"),
        P("batch", "seq"),
        P("batch", "seq", None),
    )
    return jax.shard_map(
        local,
        mesh=mesh,
        in_specs=placed,
        out_specs=(P("batch", "seq", None), P("batch", "seq", None), P("seq", None)),
        check_vma=False,
    )
```

```python
import functools

import jax
import jax.numpy as jnp
from jax import lax
from jax.experimental import pallas as pl
from jax.experimental.pallas import tpu as pltpu
from jax.sharding import PartitionSpec as P

HEADS = 16
KV_HEADS = 8
HEAD = 128
TOK = 128
D = 4608
XROWS = D // 4
QROWS = D // 16
PIECE = QROWS // 8

SCALE = 144.0 ** (-0.5)
LOG2E = 1.4426950408889634

MESH = pl.DeviceIdType.MESH
F32 = jnp.float32
BF16 = jnp.bfloat16

RELS = ((0, 1), (1, 0), (1, 1), (3, 0), (3, 1), (2, 0), (2, 1))
STEPS = (1, 3, 2)


def dot(a, b):
    return lax.dot_general(a, b, (((1,), (0,)), ((), ())), preferred_element_type=F32)


def dot_nt(a, b):
    return lax.dot_general(a, b, (((1,), (1,)), ((), ())), preferred_element_type=F32)


def kernel(
    q_hbm, do_hbm, o_hbm, k_hbm, v_hbm, ln_hbm, n_hbm, slab_ref,
    gq_ref, gk_ref, w_ref,
    q_ref, do_ref, o_ref, k_ref, v_ref, ln_ref, n_ref, in_s, pos_s, pos_r, aux_s, aux_r, q_r, do_r, kv_r, nt_s, nt_r, kt, dqt, acc, dkv_s, dkv_r,
    dvg, dq_s, dk_s, wy_s, wy_r, wz_s, wz_r, mid, wa_s, wf,
    x_ss, x_rs, x_ls, y_ss, y_rs, n_ss, n_rs, n_ls, p_ss, p_rs, dy_ss, dy_rs, dv_ss, dv_rs,
    g_ss, g_rs, g_ls, wy_ss, wy_rs, wz_ss, wz_rs, wm_ss, wm_rs, wo_ss, wo_rs, wa_ss, wa_rs,
):
    seq = lax.axis_index("seq")
    batch = lax.axis_index("batch")
    x, yh, c = seq // 4, (seq // 2) % 2, seq % 2
    yl, z = batch // 8, batch % 8
    y = 2 * yh + yl

    def device(x_, y_, c_, z_):
        return {"seq": 4 * x_ + 2 * (y_ // 2) + c_, "batch": 8 * (y_ % 2) + z_}

    def along_x(step):
        return (x + step) % 4

    def remote(src, dst, ss, rs, to):
        copy = pltpu.make_async_remote_copy(
            src_ref=src, dst_ref=dst, send_sem=ss, recv_sem=rs,
            device_id=to, device_id_type=MESH,
        )
        copy.start()
        return copy

    def keep(src, dst, sem):
        copy = pltpu.make_async_copy(src, dst, sem)
        copy.start()
        return copy

    g = 2 * x + c
    partner = device(x, (y + 2) % 4, c, z)
    peers = [device(along_x(dx), y, (c + dc) % 2, z) for dx, dc in RELS]
    slots = [2 * along_x(dx) + (c + dc) % 2 for dx, dc in RELS]
    sources = [2 * along_x(4 - dx) + (c + dc) % 2 for dx, dc in RELS]

    staged = [
        keep(source, target, in_s.at[i])
        for i, (source, target) in enumerate((
            (k_hbm, k_ref), (v_hbm, v_ref), (do_hbm, do_ref), (o_hbm, o_ref),
            (ln_hbm, ln_ref), (q_hbm, q_ref), (n_hbm, n_ref),
        ))
    ]
    pos_s[...] = jnp.full((8, TOK), slab_ref[0, 0] * TOK, jnp.int32).astype(F32)

    barrier = pltpu.get_barrier_semaphore()
    for to in peers:
        pl.semaphore_signal(barrier, inc=1, device_id=to, device_id_type=MESH)
    for step in STEPS:
        to = device(x, (y + step) % 4, c, z)
        pl.semaphore_signal(barrier, inc=1, device_id=to, device_id_type=MESH)
    for dyl in range(2):
        for dc in range(2):
            for dz in range(8):
                if dyl + dc + dz > 0:
                    to = device(x, 2 * yh + (yl + dyl) % 2, (c + dc) % 2, (z + dz) % 8)
                    pl.semaphore_signal(barrier, inc=1, device_id=to, device_id_type=MESH)
    pl.semaphore_wait(barrier, 41)

    staged[0].wait()
    staged[1].wait()

    def columns(ref, slot, width):
        return ref.at[:, pl.ds(pl.multiple_of(slot * width, width), width)]

    first, own_first = [], [
        keep(columns(k_ref, g, HEAD), kv_r.at[0, 0, g], x_ls.at[0]),
        keep(columns(v_ref, g, HEAD), kv_r.at[0, 1, g], x_ls.at[1]),
        keep(pos_s, pos_r.at[0, g], x_ls.at[2]),
    ]
    for r, to in enumerate(peers):
        first.append([
            remote(columns(k_ref, slots[r], HEAD), kv_r.at[0, 0, g], x_ss.at[0, r], x_rs.at[0, r], to),
            remote(columns(v_ref, slots[r], HEAD), kv_r.at[0, 1, g], x_ss.at[1, r], x_rs.at[1, r], to),
            remote(pos_s, pos_r.at[0, g], x_ss.at[2, r], x_rs.at[2, r], to),
        ])

    for copy in staged[2:6]:
        copy.wait()
    lane = lax.broadcasted_iota(jnp.int32, (1, TOK), 1).astype(F32)
    here = pos_s[0:1, :] + lane

    def delta_of(h, carry):
        rows = []
        for e in range(2):
            at = pl.ds(pl.multiple_of((2 * h + e) * HEAD, HEAD), HEAD)
            both = do_ref[:, at].astype(F32) * o_ref[:, at].astype(F32)
            rows.append(jnp.sum(both.T, axis=0, keepdims=True))
        norms = ln_ref[pl.ds(2 * h, 2), :] * LOG2E
        aux_s[h] = jnp.concatenate([norms, *rows, here, jnp.zeros((3, TOK), F32)], axis=0)
        return carry

    lax.fori_loop(0, KV_HEADS, delta_of, 0)

    second, own_second = [], [
        keep(aux_s.at[g], aux_r.at[0], x_ls.at[3]),
        keep(columns(q_ref, g, 2 * HEAD), q_r.at[0], x_ls.at[4]),
        keep(columns(do_ref, g, 2 * HEAD), do_r.at[0], x_ls.at[5]),
    ]
    for r, to in enumerate(peers):
        second.append([
            remote(columns(q_ref, slots[r], 2 * HEAD), q_r.at[r + 1], x_ss.at[4, r], x_rs.at[4, r], to),
            remote(columns(do_ref, slots[r], 2 * HEAD), do_r.at[r + 1], x_ss.at[5, r], x_rs.at[5, r], to),
            remote(aux_s.at[slots[r]], aux_r.at[r + 1], x_ss.at[3, r], x_rs.at[3, r], to),
        ])

    passed = []

    def pass_on(slot, r):
        passed.append(remote(kv_r.at[0, :, slot], kv_r.at[1, :, slot], y_ss.at[0, r], y_rs.at[0, r], partner))
        passed.append(remote(pos_r.at[0, slot], pos_r.at[1, slot], y_ss.at[1, r], y_rs.at[1, r], partner))

    for copy in own_first:
        copy.wait()
    pass_on(g, 7)

    for r in range(7):
        for copy in first[r]:
            copy.wait_recv()
        pass_on(sources[r], r)

    staged[6].wait()

    def turn(b, carry):
        at = pl.ds(pl.multiple_of(b * 128, 128), 128)
        nt_s[at, :] = n_ref[:, at].astype(F32).T.astype(BF16)
        return carry

    lax.fori_loop(0, D // 128, turn, 0)

    def x_rows(step):
        return nt_s.at[pl.ds(pl.multiple_of(along_x(step) * XROWS, 128), XROWS), :]

    inputs = [keep(x_rows(0), nt_r.at[g], n_ls)]
    for i, step in enumerate(STEPS):
        inputs.append(
            remote(x_rows(step), nt_r.at[g], n_ss.at[i], n_rs.at[i], device(along_x(step), y, c, z))
        )

    key_at = lax.broadcasted_iota(jnp.int32, (TOK, TOK), 0).astype(F32)

    def start(half, b):
        for k in range(4):
            kt[half, b, :, 128 * k : 128 * k + 128] = kv_r[half, 0, 4 * b + k].astype(F32).T.astype(BF16)
        acc[half, b] = jnp.zeros((2, 512, HEAD), F32)

    def block(half, b, low, high, fresh=False):
        def step(j, carry):
            queries = jnp.concatenate([q_r[j, :, :HEAD], q_r[j, :, HEAD:]], axis=0)
            grads = jnp.concatenate([do_r[j, :, :HEAD], do_r[j, :, HEAD:]], axis=0)
            aux = aux_r[j]
            norms = jnp.concatenate([aux[0:1], aux[1:2]], axis=1)
            delta = jnp.concatenate([aux[2:3], aux[3:4]], axis=1)
            query_pos = aux[4:5]
            keys = kv_r[half, 0, 4 * b : 4 * b + 4].reshape(512, HEAD)
            values = kv_r[half, 1, 4 * b : 4 * b + 4].reshape(512, HEAD)
            scores = dot_nt(keys, queries)
            dprob = dot_nt(values, grads)
            probs, dscores = [], []
            for k in range(4):
                rows = slice(128 * k, 128 * k + 128)
                ahead = query_pos - pos_r[half, 4 * b + k][0:1]
                allowed = ahead >= key_at
                prob = jnp.exp2(scores[rows] * (SCALE * LOG2E) - norms)
                prob = jnp.concatenate(
                    [jnp.where(allowed, prob[:, :128], 0.0), jnp.where(allowed, prob[:, 128:], 0.0)], axis=1
                )
                probs.append(prob.astype(BF16))
                dscores.append((prob * (dprob[rows] - delta)).astype(BF16))
            prob = jnp.concatenate(probs, axis=0)
            dscore = jnp.concatenate(dscores, axis=0)
            acc[half, b, 0] += dot(dscore, queries)
            acc[half, b, 1] += dot(prob, grads)
            term = dot(kt[half, b], dscore)
            if fresh:
                dqt[j] = term
            else:
                dqt[j] += term
            return carry

        lax.fori_loop(low, high, step, 0, unroll=2 if high - low != 8 else 4)

    across = {}

    def send_across(b, part):
        dkv_s[b, part] = acc[1, b, part].astype(BF16)
        across[b, part] = remote(
            dkv_s.at[b, part], dkv_r.at[b, part], dy_ss.at[b, part], dy_rs.at[b, part], partner
        )

    values_out = {}

    def finish_values(b):
        across[b, 1].wait_recv()
        dvg[0, 512 * b : 512 * b + 512] = (acc[0, b, 1] + dkv_r[b, 1].astype(F32)).astype(BF16)

    def send_values(b, i):
        rows = slice(512 * b, 512 * b + 512)
        values_out[b, i] = remote(
            dvg.at[0, rows], dvg.at[i + 1, rows], dv_ss.at[b, i], dv_rs.at[b, i],
            device(along_x(STEPS[i]), y, c, z),
        )

    def finish_keys(b):
        across[b, 0].wait_recv()
        keys_done = (SCALE * (acc[0, b, 0] + dkv_r[b, 0].astype(F32))).astype(BF16)
        dk_s[4 * b : 4 * b + 4] = keys_done.reshape(4, 128, HEAD)

    other = device(x, y, (c + 1) % 2, z)
    shared = []

    def share(i, step):
        if i == 0:
            inputs[0].wait()
        else:
            inputs[i].wait_recv()
        j = 2 * along_x(step) + c
        shared.append(remote(nt_r.at[j], nt_r.at[j], p_ss.at[i], p_rs.at[i], other))

    def arrived(low, high):
        for r in range(low, high):
            for copy in second[r]:
                copy.wait_recv()

    start(0, 0)
    for copy in own_second:
        copy.wait()
    arrived(0, 5)
    block(0, 0, 0, 6, fresh=True)
    for copy in passed:
        copy.wait_recv()
    start(1, 0)
    block(1, 0, 0, 6)
    arrived(5, 7)
    block(1, 0, 6, 8, fresh=True)
    send_across(0, 1)
    start(1, 1)
    block(1, 1, 0, 8)
    send_across(1, 1)
    send_across(0, 0)
    send_across(1, 0)
    share(0, 0)
    block(0, 0, 6, 8)
    finish_values(0)
    send_values(0, 0)
    send_values(0, 1)
    start(0, 1)
    block(0, 1, 0, 8)
    finish_values(1)
    send_values(1, 0)
    send_values(1, 1)
    send_values(0, 2)
    send_values(1, 2)
    share(1, 3)
    share(2, 1)
    share(3, 2)

    def queries_done(j, carry):
        dq_s[j] = jnp.concatenate(
            [(SCALE * dqt[j, :, :128]).T, (SCALE * dqt[j, :, 128:]).T], axis=1
        ).astype(BF16)
        return carry

    lax.fori_loop(0, 8, queries_done, 0)

    for copy in shared:
        copy.wait_recv()

    back = []

    def send_back():
        finish_keys(0)
        finish_keys(1)
        back.extend([
            keep(dk_s.at[g], columns(gk_ref, g, HEAD), g_ls.at[0]),
            keep(dq_s.at[0], columns(gq_ref, g, 2 * HEAD), g_ls.at[1]),
        ])
        for r, (dx, dc) in enumerate(RELS):
            to = device(along_x(4 - dx), y, (c + dc) % 2, z)
            back.append(remote(dk_s.at[sources[r]], columns(gk_ref, g, HEAD), g_ss.at[0, r], g_rs.at[0, r], to))
            back.append(remote(dq_s.at[r + 1], columns(gq_ref, g, 2 * HEAD), g_ss.at[1, r], g_rs.at[1, r], to))

    over_y = []

    def multiply(i):
        if i > 0:
            values_out[0, i - 1].wait_recv()
            values_out[1, i - 1].wait_recv()

        def quarter(t):
            at = pl.ds(pl.multiple_of(t * QROWS, 32), QROWS)
            total = None
            for j in range(4):
                left = jnp.concatenate([nt_r[2 * j, at, :], nt_r[2 * j + 1, at, :]], axis=1)
                term = dot(left, dvg[i, 256 * j : 256 * j + 256])
                total = term if total is None else total + term
            wy_s[i, t] = total.astype(BF16)

        over_y.append([])
        for k, step in enumerate((1, 3, 2)):
            t = (y + step) % 4
            quarter(t)
            over_y[i].append(
                remote(wy_s.at[i, t], wy_r.at[i, k], wy_ss.at[i, k], wy_rs.at[i, k], device(x, t, c, z))
            )
        quarter(y)

    over_z = []

    def reduce_y(i):
        total = wy_s[i, y].astype(F32)
        for k in range(3):
            over_y[i][k].wait_recv()
            total = total + wy_r[i, k].astype(F32)
        for k in range(8):
            wz_s[i, k] = total[PIECE * k : PIECE * k + PIECE].astype(BF16)
        over_z.append([
            remote(
                wz_s.at[i, (z + k) % 8], wz_r.at[i, k - 1], wz_ss.at[i, k - 1], wz_rs.at[i, k - 1],
                device(x, y, c, (z + k) % 8),
            )
            for k in (4, 3, 5, 2, 6, 1, 7)
        ])

    def column_block(i, core):
        return 2 * along_x((0, 3, 1, 2)[i]) + core

    def sum_z(i):
        total = wz_s[i, z].astype(F32)
        for copy in over_z[i]:
            copy.wait_recv()
        for k in range(7):
            total = total + wz_r[i, k].astype(F32)
        return total.astype(BF16)

    def w_copy(t):
        dyl, dz = t // 8, t % 8
        return pltpu.make_async_remote_copy(
            src_ref=wa_s, dst_ref=wf.at[column_block(3, c), z], send_sem=wa_ss.at[t], recv_sem=wa_rs.at[c, z],
            device_id=device(x, 2 * yh + (yl + dyl) % 2, yl, (z + dz) % 8), device_id_type=MESH,
        )

    def last_z():
        wa_s[...] = sum_z(3)
        for t in (12, 4, 11, 3, 13, 5, 10, 2, 14, 6, 9, 1, 15, 7, 8):
            w_copy(t).start()
        pl.when(c != yl)(lambda: w_copy(0).start())
        pl.when(c == yl)(
            lambda: pltpu.make_async_copy(wa_s, wf.at[column_block(3, c), z], wa_rs.at[c, z]).start()
        )

    gathered = []

    def reduce_z(i):
        mid[i, z] = sum_z(i)
        gathered.append([
            remote(
                mid.at[i, z], mid.at[i, z], wm_ss.at[i, k - 1], wm_rs.at[i, k - 1],
                device(x, y, c, (z + k) % 8),
            )
            for k in (4, 3, 5, 2, 6, 1, 7)
        ])

    def near_copy(i):
        block = column_block(i, c)
        return pltpu.make_async_remote_copy(
            src_ref=mid.at[i], dst_ref=wf.at[block], send_sem=wo_ss.at[i, 0], recv_sem=wo_rs.at[block],
            device_id=device(x, y, yl, z), device_id_type=MESH,
        )

    handed = []

    def hand_over(i):
        for copy in gathered[i]:
            copy.wait_recv()
        block = column_block(i, c)
        handed.append(
            remote(
                mid.at[i], wf.at[block], wo_ss.at[i, 1], wo_rs.at[block],
                device(x, 2 * yh + (yl + 1) % 2, yl, z),
            )
        )
        pl.when(c != yl)(lambda: near_copy(i).start())
        pl.when(c == yl)(lambda: pltpu.make_async_copy(mid.at[i], wf.at[block], wo_rs.at[block]).start())

    multiply(0)
    multiply(1)
    multiply(2)
    reduce_y(0)
    multiply(3)
    send_back()
    reduce_y(1)
    reduce_z(0)
    reduce_y(2)
    reduce_z(1)
    reduce_y(3)
    reduce_z(2)
    hand_over(0)
    last_z()
    hand_over(1)
    hand_over(2)

    for copy in back:
        if copy is back[0] or copy is back[1]:
            copy.wait()
        else:
            copy.wait_recv()

    for i in range(4):
        for core in range(2):
            block = column_block(i, core)
            at = pl.ds(pl.multiple_of(128 * block, 128), 128)
            if i < 3:
                pltpu.make_async_copy(mid.at[i], wf.at[block], wo_rs.at[block]).wait()
            for k in range(8):
                if i == 3:
                    pltpu.make_async_copy(wa_s, wf.at[block, k], wa_rs.at[core, k]).wait()
                w_ref[PIECE * k : PIECE * k + PIECE, at] = wf[block, k].astype(F32)

    for group in first + second + over_y + over_z + gathered:
        for copy in group:
            copy.wait_send()
    for copy in passed + inputs[1:] + shared + [*across.values(), *values_out.values()] + back[2:] + handed:
        copy.wait_send()
    for t in range(1, 16):
        w_copy(t).wait_send()
    pl.when(c != yl)(lambda: w_copy(0).wait_send())
    for i in range(3):
        pl.when(c != yl)(lambda: near_copy(i).wait_send())


def write(gq_ref, gk_ref, w_ref, gq_hbm, gk_hbm, w_hbm, sems):
    copies = [
        pltpu.make_async_copy(source, target, sems.at[i])
        for i, (source, target) in enumerate(((w_ref, w_hbm), (gq_ref, gq_hbm), (gk_ref, gk_hbm)))
    ]
    for copy in copies:
        copy.start()
    for copy in copies:
        copy.wait()


def local(
    query_rows, key_rows, value_rows, attn_output, output_grad, log_norm, slab_order, normed_input
):
    vmem = pl.BlockSpec(memory_space=pltpu.VMEM)
    smem = pl.BlockSpec(memory_space=pltpu.SMEM)
    dma = pltpu.SemaphoreType.DMA
    shapes = (
        jax.ShapeDtypeStruct((TOK, HEADS * HEAD), BF16),
        jax.ShapeDtypeStruct((TOK, KV_HEADS * HEAD), BF16),
        jax.ShapeDtypeStruct((QROWS, KV_HEADS * HEAD), F32),
    )
    results = pl.pallas_call(
        kernel,
        name="step",
        out_shape=shapes,
        in_specs=[pl.BlockSpec(memory_space=pltpu.HBM)] * 7 + [smem],
        out_specs=(vmem, vmem, vmem),
        scratch_shapes=[
            pltpu.VMEM((TOK, HEADS * HEAD), BF16),
            pltpu.VMEM((TOK, HEADS * HEAD), BF16),
            pltpu.VMEM((TOK, HEADS * HEAD), BF16),
            pltpu.VMEM((TOK, KV_HEADS * HEAD), BF16),
            pltpu.VMEM((TOK, KV_HEADS * HEAD), BF16),
            pltpu.VMEM((HEADS, TOK), F32),
            pltpu.VMEM((TOK, D), BF16),
            dma((7,)),
            pltpu.VMEM((8, TOK), F32),
            pltpu.VMEM((2, 8, 8, TOK), F32),
            pltpu.VMEM((8, 8, TOK), F32),
            pltpu.VMEM((8, 8, TOK), F32),
            pltpu.VMEM((8, TOK, 2 * HEAD), BF16),
            pltpu.VMEM((8, TOK, 2 * HEAD), BF16),
            pltpu.VMEM((2, 2, 8, TOK, HEAD), BF16),
            pltpu.VMEM((D, TOK), BF16),
            pltpu.VMEM((8, XROWS, TOK), BF16),
            pltpu.VMEM((2, 2, HEAD, 512), BF16),
            pltpu.VMEM((8, HEAD, 2 * TOK), F32),
            pltpu.VMEM((2, 2, 2, 512, HEAD), F32),
            pltpu.VMEM((2, 2, 512, HEAD), BF16),
            pltpu.VMEM((2, 2, 512, HEAD), BF16),
            pltpu.VMEM((4, 1024, HEAD), BF16),
            pltpu.VMEM((8, TOK, 2 * HEAD), BF16),
            pltpu.VMEM((8, TOK, HEAD), BF16),
            pltpu.VMEM((4, 4, QROWS, HEAD), BF16),
            pltpu.VMEM((4, 3, QROWS, HEAD), BF16),
            pltpu.VMEM((4, 8, PIECE, HEAD), BF16),
            pltpu.VMEM((4, 7, PIECE, HEAD), BF16),
            pltpu.VMEM((3, 8, PIECE, HEAD), BF16),
            pltpu.VMEM((PIECE, HEAD), BF16),
            pltpu.VMEM((8, 8, PIECE, HEAD), BF16),
            dma((6, 7)), dma((6, 7)), dma((6,)),
            dma((2, 8)), dma((2, 8)),
            dma((3,)), dma((3,)), dma,
            dma((4,)), dma((4,)),
            dma((2, 2)), dma((2, 2)),
            dma((2, 3)), dma((2, 3)),
            dma((2, 7)), dma((2, 7)), dma((2,)),
            dma((4, 3)), dma((4, 3)),
            dma((4, 7)), dma((4, 7)),
            dma((3, 7)), dma((3, 7)), dma((3, 2)), dma((8,)),
            dma((16,)), dma((2, 8)),
        ],
        compiler_params=pltpu.CompilerParams(
            collective_id=0, has_side_effects=True, vmem_limit_bytes=44 * 2**20
        ),
    )(
        *(
            pltpu.with_memory_space_constraint(part[0], pltpu.HBM)
            for part in (query_rows, output_grad, attn_output, key_rows, value_rows, log_norm, normed_input)
        ),
        slab_order,
    )
    grad_query, grad_key, weight = pl.pallas_call(
        write,
        name="write",
        out_shape=shapes,
        in_specs=[vmem] * 3,
        out_specs=[pl.BlockSpec(memory_space=pltpu.HBM)] * 3,
        scratch_shapes=[dma((3,))],
        compiler_params=pltpu.CompilerParams(vmem_limit_bytes=2**20),
    )(*results)
    return grad_query[None], grad_key[None], weight


def solution(mesh):
    placed = (
        P("batch", "seq", None),
        P("batch", "seq", None),
        P("batch", "seq", None),
        P("batch", "seq", None),
        P("batch", "seq", None),
        P("batch", None, "seq"),
        P("batch", "seq"),
        P("batch", "seq", None),
    )
    return jax.shard_map(
        local,
        mesh=mesh,
        in_specs=placed,
        out_specs=(P("batch", "seq", None), P("batch", "seq", None), P("seq", None)),
        check_vma=False,
    )
```
